128 devices in a mesh: mp: 1, dp: 128 (over z, y, x, core).
Axes of the slice: x: 4, y: 4, z: 4, core: 2. Of those that a mesh axis runs over, the one named last changes fastest.
Arguments:
- grad_partial: float32 [128, 1, 2048, 1024], P(('mp', 'dp'))
- momentum: float32 [1, 2048, 1024], P('mp', 'dp')
- weight: float32 [1, 2048, 1024], P('mp', 'dp')
Outputs:
- output 1: float32 [1, 2048, 1024], P('mp', 'dp')
- output 2: float32 [1, 2048, 1024], P('mp', 'dp')
- output 3: bfloat16 [1, 2048, 1024], P('mp')
All inputs are finite; a program needn't handle non-finite values.
Results may differ from the reference program's by a relative error of at most 0.0159465.
Values are sent between devices in bfloat16 or wider.
A program may use at most 1 GiB of HBM per device.

```python
import math
import jax
import jax.numpy as jnp
from jax import lax

GROUP_SIZE = 128
NUM_MATS = 1
MAT_ROWS = 2048
MAT_COLS = 1024
NS_STEPS = 5
MOMENTUM = 0.95
LEARN_RATE = 2.0
WEIGHT_DECAY = 0.25
COEF_A = 3.4445
COEF_B = -4.7750
COEF_C = 2.0315


def setup_inputs(seed: int = 0, part: int = 0) -> dict:
    part_key = jax.random.fold_in(jax.random.key(seed), part)
    key_grad, key_moment, key_weight = jax.random.split(part_key, 3)
    mat_shape = (NUM_MATS, MAT_ROWS, MAT_COLS)
    grad_partial = jax.random.normal(key_grad, (GROUP_SIZE,) + mat_shape, jnp.float32) * math.sqrt(GROUP_SIZE)
    momentum = jax.random.normal(key_moment, mat_shape, jnp.float32)
    weight = jax.random.normal(key_weight, mat_shape, jnp.float32)
    return {'grad_partial': grad_partial, 'momentum': momentum, 'weight': weight}


def newton_schulz(direction):
    num_rows, num_cols = direction.shape
    as_float = direction.astype(jnp.float32)
    norm = jnp.sqrt(jnp.sum(as_float * as_float))
    ortho = (as_float / (norm + 1e-7)).astype(jnp.bfloat16)
    if num_rows > num_cols:
        ortho = ortho.T
    for _ in range(NS_STEPS):
        gram = jnp.dot(ortho, ortho.T, preferred_element_type=jnp.float32).astype(jnp.bfloat16)
        gram_sq = jnp.dot(gram, gram, preferred_element_type=jnp.float32)
        poly = (COEF_B * gram.astype(jnp.float32) + COEF_C * gram_sq).astype(jnp.bfloat16)
        ortho = (COEF_A * ortho.astype(jnp.float32) + jnp.dot(poly, ortho, preferred_element_type=jnp.float32)).astype(jnp.bfloat16)
    if num_rows > num_cols:
        ortho = ortho.T
    return ortho


def reference(grad_partial, momentum, weight):
    grad = jnp.sum(grad_partial, axis=0) / GROUP_SIZE
    new_momentum = MOMENTUM * momentum + grad
    direction = (grad + MOMENTUM * new_momentum).astype(jnp.bfloat16)
    ortho = lax.map(newton_schulz, direction)
    scale = 0.2 * math.sqrt(max(MAT_ROWS, MAT_COLS))
    new_weight = weight - LEARN_RATE * (scale * ortho.astype(jnp.float32) + WEIGHT_DECAY * weight)
    return new_momentum, new_weight, new_weight.astype(jnp.bfloat16)
```

```python
import math
import jax
import jax.numpy as jnp
from jax import lax
from jax.experimental import pallas as pl
from jax.experimental.pallas import tpu as pltpu
from jax.sharding import PartitionSpec as P

MOMENTUM = 0.95
LEARN_RATE = 2.0
WEIGHT_DECAY = 0.25
NS_STEPS = 5
COEF_A = 3.4445
COEF_B = -4.7750
COEF_C = 2.0315

MESH = pl.DeviceIdType.MESH
RING = 4
CHIPS = 64
GROUP = 128
SLAB = 16
COLS = 1024
ROWS = 2048
Z, Y, X = 0, 1, 2
PARTS = ((0, 384, (X, Y, Z)), (384, 384, (Y, Z, X)), (768, 256, (Z, X, Y)))


class Place:
    def __init__(self):
        me = lax.axis_index('dp')
        self.core = lax.rem(me, 2)
        chip = lax.div(me, 2)
        self.xyz = (lax.div(chip, 16), lax.rem(lax.div(chip, 4), 4), lax.rem(chip, 4))

    def index(self, xyz, core):
        return ((xyz[0] * RING + xyz[1]) * RING + xyz[2]) * 2 + core

    def shifted(self, axis, by):
        return lax.rem(self.xyz[axis] + (by % RING), RING)

    def neighbour(self, axis, by):
        xyz = list(self.xyz)
        xyz[axis] = self.shifted(axis, by)
        return {'dp': self.index(xyz, self.core)}

    def partner(self):
        return {'dp': self.index(self.xyz, 1 - self.core)}


def greet(place):
    barrier = pltpu.get_barrier_semaphore()
    peers = [place.partner()] + [place.neighbour(a, s) for a in (Z, Y, X) for s in (1, -1, 2)]
    for peer in peers:
        pl.semaphore_signal(barrier, inc=1, device_id=peer, device_id_type=MESH)
    pl.semaphore_wait(barrier, len(peers))


def at(fixed, rows, cols):
    return tuple(fixed.get(a, slice(None)) for a in (Z, Y, X)) + (rows, cols)


def send(src, dst, ssem, rsem, peer):
    copy = pltpu.make_async_remote_copy(src_ref=src, dst_ref=dst, send_sem=ssem, recv_sem=rsem, device_id=peer, device_id_type=MESH)
    copy.start()
    return copy


ALL = slice(None)
LOW, HIGH = pl.ds(0, 8), pl.ds(8, 8)


def reduce_phase(place, acc, ring_refs, ssem, rsem, part, phase, ready):
    first, width, order = PARTS[part]
    axis = order[phase]
    cols = pl.ds(first, width)
    near_l, near_r, far_l, far_r = ring_refs
    fixed = {a: place.xyz[a] for a in order[:phase]}
    right, left = place.neighbour(axis, 1), place.neighbour(axis, -1)

    def chunk(by, rows):
        return at({**fixed, axis: place.shifted(axis, by)}, rows, cols)

    def sub(rows):
        return tuple(ALL for _ in range(2 - phase)) + (rows, cols)

    started = []
    sems = lambda i: (ssem.at[part, phase, i], rsem.at[part, phase, i])
    ready(2)
    started.append(send(acc.at[chunk(2, LOW)], far_l.at[sub(ALL)], *sems(0), right))
    started.append(send(acc.at[chunk(2, HIGH)], far_r.at[sub(ALL)], *sems(1), left))
    yield
    ready(1)
    started.append(send(acc.at[chunk(1, HIGH)], near_l.at[sub(HIGH)], *sems(2), right))
    yield
    ready(-1)
    started.append(send(acc.at[chunk(-1, LOW)], near_r.at[sub(LOW)], *sems(3), left))
    yield
    started[0].wait_recv()
    acc[chunk(1, LOW)] += far_l[sub(ALL)]
    started.append(send(acc.at[chunk(1, LOW)], near_l.at[sub(LOW)], *sems(4), right))
    yield
    started[1].wait_recv()
    acc[chunk(-1, HIGH)] += far_r[sub(ALL)]
    started.append(send(acc.at[chunk(-1, HIGH)], near_r.at[sub(HIGH)], *sems(5), left))
    yield
    ready(0)
    yield
    for i in (2, 3, 4, 5):
        started[i].wait_recv()
    acc[chunk(0, ALL)] += near_l[sub(ALL)] + near_r[sub(ALL)]
    return started


def gather_phase(place, buf, ssem, rsem, part, phase, on_piece):
    first, width, order = PARTS[part]
    axis = order[phase]
    cols = pl.ds(first, width)
    fixed = {a: place.xyz[a] for a in order[:phase]}
    right, left, across = place.neighbour(axis, 1), place.neighbour(axis, -1), place.neighbour(axis, 2)
    free = [a for a in (Z, Y, X) if a in order[phase + 1:]]
    sems = lambda i: (ssem.at[part, phase, i], rsem.at[part, phase, i])

    def chunk(by, half=None):
        where = {**fixed, axis: place.shifted(axis, by)}
        if half is not None:
            where[free[0]] = pl.ds(2 * half, 2)
        return at(where, ALL, cols)

    def recv(i, by, half=None):
        there = buf.at[chunk(by, half)]
        pltpu.make_async_remote_copy(src_ref=there, dst_ref=there, send_sem=ssem.at[part, phase, i], recv_sem=rsem.at[part, phase, i], device_id=right, device_id_type=MESH).wait_recv()

    started = []
    mine = buf.at[chunk(0)]
    started.append(send(mine, mine, *sems(0), right))
    started.append(send(mine, mine, *sems(1), left))
    if not free:
        started.append(send(mine, mine, *sems(2), across))
        on_piece(0, chunk(0))
        yield
        recv(0, -1)
        recv(1, 1)
        recv(2, 2)
    else:
        on_piece(0, chunk(0))
        yield
        recv(0, -1)
        there = buf.at[chunk(-1, 0)]
        started.append(send(there, there, *sems(2), right))
        on_piece(1, chunk(-1))
        yield
        recv(1, 1)
        there = buf.at[chunk(1, 1)]
        started.append(send(there, there, *sems(3), left))
        on_piece(2, chunk(1))
        yield
        recv(2, 2, 0)
        on_piece(3, chunk(2, 0))
        yield
        recv(3, 2, 1)
        on_piece(4, chunk(2, 1))
    return started


def run_together(generators):
    started, live = [], list(generators)
    while live:
        left = []
        for g in live:
            try:
                next(g)
                left.append(g)
            except StopIteration as stop:
                started.extend(stop.value)
        live = left
    return started


def comm_kernel(grad, momentum, new_momentum, mine, other, acc, half, *scratch):
    ring = scratch[:12]
    load_sem, pair_ssem, pair_rsem, rs_ssem, rs_rsem, ag_ssem, ag_rsem, fw_ssem, fw_rsem = scratch[12:]
    place = Place()
    stages = (2, 1, -1, 0)
    loads, swaps = {}, {}
    for s, by in enumerate(stages):
        for p, (first, width, order) in enumerate(PARTS):
            axis = order[0]
            block = {axis: place.shifted(axis, by)}
            z, y, x, r, c = at(block, ALL, pl.ds(first, width))
            loads[p, by] = pltpu.make_async_copy(grad.at[z, y, x, place.core, r, c], acc.at[z, y, x, r, c], load_sem.at[p, s])
            loads[p, by].start()
    greet(place)
    for s, by in enumerate(stages):
        for p, (first, width, order) in enumerate(PARTS):
            axis = order[0]
            block = {axis: place.shifted(axis, by)}
            z, y, x, r, c = at(block, ALL, pl.ds(first, width))
            swaps[p, by] = send(grad.at[z, y, x, 1 - place.core, r, c], half.at[z, y, x, r, c], pair_ssem.at[p, s], pair_rsem.at[p, s], place.partner())

    def ready(part):
        def chunk_ready(by):
            first, width, order = PARTS[part]
            here = at({order[0]: place.shifted(order[0], by)}, ALL, pl.ds(first, width))
            loads[part, by].wait()
            swaps[part, by].wait_recv()
            acc[here] += half[here]
        return chunk_ready

    sent = list(swaps.values())
    for phase in range(3):
        sent += run_together([reduce_phase(place, acc, ring[4 * phase:4 * phase + 4], rs_ssem, rs_rsem, p, phase, ready(p) if phase == 0 else (lambda by: None)) for p in range(3)])

    z, y, x = place.xyz
    g = acc[z, y, x] / GROUP
    mom = MOMENTUM * momentum[...] + g
    new_momentum[...] = mom
    mine[z, y, x] = (g + MOMENTUM * mom).astype(jnp.bfloat16)

    forwards = []

    def forward(part):
        def on_piece(i, where):
            forwards.append(send(mine.at[where], other.at[where], fw_ssem.at[part, i], fw_rsem.at[part, i], place.partner()))
        return on_piece

    for phase in (2, 1, 0):
        sent += run_together([gather_phase(place, mine, ag_ssem, ag_rsem, p, phase, forward(p) if phase == 0 else (lambda i, w: None)) for p in range(3)])
    for copy in forwards:
        copy.wait_recv()
    for copy in sent + forwards:
        copy.wait_send()


def comm(grad, momentum):
    ring = []
    for lead in ((RING, RING), (RING,), ()):
        ring += [pltpu.VMEM(lead + (SLAB, COLS), jnp.float32)] * 2 + [pltpu.VMEM(lead + (8, COLS), jnp.float32)] * 2
    dma = pltpu.SemaphoreType.DMA
    cube = (RING, RING, RING, SLAB, COLS)
    vmem = pl.BlockSpec(memory_space=pltpu.VMEM)
    return pl.pallas_call(
        comm_kernel,
        out_shape=(jax.ShapeDtypeStruct((SLAB, COLS), jnp.float32), jax.ShapeDtypeStruct(cube, jnp.bfloat16), jax.ShapeDtypeStruct(cube, jnp.bfloat16)),
        in_specs=[pl.BlockSpec(memory_space=pl.ANY), vmem],
        out_specs=(vmem, vmem, vmem),
        scratch_shapes=[pltpu.VMEM(cube, jnp.float32), pltpu.VMEM(cube, jnp.float32), *ring,
                        dma((3, 4)), dma((3, 4)), dma((3, 4)), dma((3, 3, 6)), dma((3, 3, 6)), dma((3, 3, 4)), dma((3, 3, 4)), dma((3, 5)), dma((3, 5))],
        compiler_params=pltpu.CompilerParams(collective_id=0, has_side_effects=True, vmem_limit_bytes=60 << 20),
        name='reduce_gather',
    )(grad, momentum)


def orthogonalise(update):
    as_float = update.astype(jnp.float32)
    sq_norm = jnp.sum(as_float * as_float)
    ortho = (as_float / (jnp.sqrt(sq_norm) + 1e-7)).astype(jnp.bfloat16)
    for _ in range(NS_STEPS):
        gram = jnp.einsum('lk,lj->kj', ortho, ortho, preferred_element_type=jnp.float32).astype(jnp.bfloat16)
        gram_sq = jnp.einsum('kj,ji->ki', gram, gram, preferred_element_type=jnp.float32)
        poly = (COEF_B * gram.astype(jnp.float32) + COEF_C * gram_sq).astype(jnp.bfloat16)
        ortho = (COEF_A * ortho.astype(jnp.float32) + jnp.einsum('kj,lj->lk', poly, ortho, preferred_element_type=jnp.float32)).astype(jnp.bfloat16)
    return ortho


def solution(mesh):
    def local_step(grad_part, momentum, weight):
        grad = grad_part.reshape(RING, RING, RING, 2, SLAB, COLS)
        new_momentum, mine, other = comm(grad, momentum[0])
        core = lax.rem(lax.axis_index('dp'), 2)
        first = core == 0
        pair = jnp.stack([jnp.where(first, mine, other), jnp.where(first, other, mine)], axis=3)
        ortho = orthogonalise(pair.reshape(ROWS, COLS))
        slab = lax.dynamic_slice(ortho, (lax.axis_index('dp') * SLAB, 0), (SLAB, COLS))
        scale = 0.2 * math.sqrt(ROWS)
        new_weight = weight - LEARN_RATE * (scale * slab.astype(jnp.float32)[None] + WEIGHT_DECAY * weight)
        weight_bf16 = lax.all_gather(new_weight.astype(jnp.bfloat16), 'dp', axis=1, tiled=True)
        return new_momentum[None], new_weight, weight_bf16

    return jax.shard_map(local_step, mesh=mesh, in_specs=(P(('mp', 'dp')), P('mp', 'dp'), P('mp', 'dp')), out_specs=(P('mp', 'dp'), P('mp', 'dp'), P('mp')), check_vma=False)
```

```python
import math
import jax
import jax.numpy as jnp
from jax import lax
from jax.experimental import pallas as pl
from jax.experimental.pallas import tpu as pltpu
from jax.sharding import PartitionSpec as P

MOMENTUM = 0.95
LEARN_RATE = 2.0
WEIGHT_DECAY = 0.25
NS_STEPS = 5
COEF_A = 3.4445
COEF_B = -4.7750
COEF_C = 2.0315

MESH = pl.DeviceIdType.MESH
RING = 4
CHIPS = 64
GROUP = 128
SLAB = 16
COLS = 1024
ROWS = 2048
Z, Y, X = 0, 1, 2
PARTS = ((0, 384, (X, Y, Z)), (384, 384, (Y, Z, X)), (768, 256, (Z, X, Y)))


class Place:
    def __init__(self):
        me = lax.axis_index('dp')
        self.core = lax.rem(me, 2)
        chip = lax.div(me, 2)
        self.xyz = (lax.div(chip, 16), lax.rem(lax.div(chip, 4), 4), lax.rem(chip, 4))

    def index(self, xyz, core):
        return ((xyz[0] * RING + xyz[1]) * RING + xyz[2]) * 2 + core

    def shifted(self, axis, by):
        return lax.rem(self.xyz[axis] + (by % RING), RING)

    def neighbour(self, axis, by):
        xyz = list(self.xyz)
        xyz[axis] = self.shifted(axis, by)
        return {'dp': self.index(xyz, self.core)}

    def partner(self):
        return {'dp': self.index(self.xyz, 1 - self.core)}


def greet(place):
    barrier = pltpu.get_barrier_semaphore()
    peers = [place.partner()] + [place.neighbour(a, s) for a in (Z, Y, X) for s in (1, -1, 2)]
    for peer in peers:
        pl.semaphore_signal(barrier, inc=1, device_id=peer, device_id_type=MESH)
    pl.semaphore_wait(barrier, len(peers))


def at(fixed, rows, cols):
    return tuple(fixed.get(a, slice(None)) for a in (Z, Y, X)) + (rows, cols)


def send(src, dst, ssem, rsem, peer):
    copy = pltpu.make_async_remote_copy(src_ref=src, dst_ref=dst, send_sem=ssem, recv_sem=rsem, device_id=peer, device_id_type=MESH)
    copy.start()
    return copy


ALL = slice(None)
LOW, HIGH = pl.ds(0, 8), pl.ds(8, 8)


def reduce_phase(place, acc, ring_refs, ssem, rsem, part, phase, ready):
    first, width, order = PARTS[part]
    axis = order[phase]
    cols = pl.ds(first, width)
    near_l, near_r, far_l, far_r = ring_refs
    fixed = {a: place.xyz[a] for a in order[:phase]}
    right, left = place.neighbour(axis, 1), place.neighbour(axis, -1)

    def chunk(by, rows):
        return at({**fixed, axis: place.shifted(axis, by)}, rows, cols)

    def sub(rows):
        return tuple(ALL for _ in range(2 - phase)) + (rows, cols)

    started = []
    sems = lambda i: (ssem.at[part, phase, i], rsem.at[part, phase, i])
    ready(2)
    started.append(send(acc.at[chunk(2, LOW)], far_l.at[sub(ALL)], *sems(0), right))
    started.append(send(acc.at[chunk(2, HIGH)], far_r.at[sub(ALL)], *sems(1), left))
    yield
    ready(1)
    started.append(send(acc.at[chunk(1, HIGH)], near_l.at[sub(HIGH)], *sems(2), right))
    yield
    ready(-1)
    started.append(send(acc.at[chunk(-1, LOW)], near_r.at[sub(LOW)], *sems(3), left))
    yield
    started[0].wait_recv()
    acc[chunk(1, LOW)] += far_l[sub(ALL)]
    started.append(send(acc.at[chunk(1, LOW)], near_l.at[sub(LOW)], *sems(4), right))
    yield
    started[1].wait_recv()
    acc[chunk(-1, HIGH)] += far_r[sub(ALL)]
    started.append(send(acc.at[chunk(-1, HIGH)], near_r.at[sub(HIGH)], *sems(5), left))
    yield
    ready(0)
    yield
    for i in (2, 3, 4, 5):
        started[i].wait_recv()
    acc[chunk(0, ALL)] += near_l[sub(ALL)] + near_r[sub(ALL)]
    return started


def gather_phase(place, buf, ssem, rsem, part, phase, on_piece):
    first, width, order = PARTS[part]
    axis = order[phase]
    cols = pl.ds(first, width)
    fixed = {a: place.xyz[a] for a in order[:phase]}
    right, left, across = place.neighbour(axis, 1), place.neighbour(axis, -1), place.neighbour(axis, 2)
    free = [a for a in (Z, Y, X) if a in order[phase + 1:]]
    sems = lambda i: (ssem.at[part, phase, i], rsem.at[part, phase, i])

    def chunk(by, half=None):
        where = {**fixed, axis: place.shifted(axis, by)}
        if half is not None:
            where[free[0]] = pl.ds(2 * half, 2)
        return at(where, ALL, cols)

    def recv(i, by, half=None):
        there = buf.at[chunk(by, half)]
        pltpu.make_async_remote_copy(src_ref=there, dst_ref=there, send_sem=ssem.at[part, phase, i], recv_sem=rsem.at[part, phase, i], device_id=right, device_id_type=MESH).wait_recv()

    started = []
    mine = buf.at[chunk(0)]
    started.append(send(mine, mine, *sems(0), right))
    started.append(send(mine, mine, *sems(1), left))
    if not free:
        started.append(send(mine, mine, *sems(2), across))
        on_piece(0, chunk(0))
        yield
        recv(0, -1)
        recv(1, 1)
        recv(2, 2)
    else:
        on_piece(0, chunk(0))
        yield
        recv(0, -1)
        there = buf.at[chunk(-1, 0)]
        started.append(send(there, there, *sems(2), right))
        on_piece(1, chunk(-1))
        yield
        recv(1, 1)
        there = buf.at[chunk(1, 1)]
        started.append(send(there, there, *sems(3), left))
        on_piece(2, chunk(1))
        yield
        recv(2, 2, 0)
        on_piece(3, chunk(2, 0))
        yield
        recv(3, 2, 1)
        on_piece(4, chunk(2, 1))
    return started


def run_together(generators):
    started, live = [], list(generators)
    while live:
        left = []
        for g in live:
            try:
                next(g)
                left.append(g)
            except StopIteration as stop:
                started.extend(stop.value)
        live = left
    return started


NT = (((1,), (1,)), ((), ()))
BLK = 256
NBLK = COLS // BLK


def dot(a, b):
    return jnp.dot(a, b, preferred_element_type=jnp.float32)


def weight_step(place, weight, full, ssem, rsem, step):
    def piece(part, phase, i):
        first, width, order = PARTS[part]
        axis = order[phase]
        cols = pl.ds(first, width)
        fixed = {a: place.xyz[a] for a in order[:phase]}
        free = [a for a in (Z, Y, X) if a in order[phase + 1:]]
        right, left, across = place.neighbour(axis, 1), place.neighbour(axis, -1), place.neighbour(axis, 2)

        def chunk(by, half=None):
            where = {**fixed, axis: place.shifted(axis, by)}
            if half is not None:
                where[free[0]] = pl.ds(2 * half, 2)
            return full.at[at(where, ALL, cols)]

        if not free:
            src_by, half, peer, from_by = ((0, None, right, -1), (0, None, left, 1), (0, None, across, 2))[i]
        else:
            src_by, half, peer, from_by = ((0, None, right, -1), (0, None, left, 1), (-1, 0, right, 2), (1, 1, left, 2))[i]
        out = chunk(src_by, half)
        src = weight.at[:, cols] if not free else out
        go = lambda: pltpu.make_async_remote_copy(src_ref=src, dst_ref=out, send_sem=ssem.at[part, phase, i], recv_sem=rsem.at[part, phase, i], device_id=peer, device_id_type=MESH)
        came = chunk(from_by, half)
        come = lambda: pltpu.make_async_remote_copy(src_ref=came, dst_ref=came, send_sem=ssem.at[part, phase, i], recv_sem=rsem.at[part, phase, i], device_id=peer, device_id_type=MESH)
        return go, come

    plan = {0: ((), (2, (0, 1, 2))), 1: ((2, (0, 1, 2)), (1, (0, 1))), 2: ((1, (0, 1)), (1, (2, 3))), 3: ((1, (2, 3)), (0, (0, 1))), 4: ((0, (0, 1)), (0, (2, 3))), 5: ((0, (2, 3)), ())}
    waits, sends = plan[step]
    if waits:
        for i in waits[1]:
            for part in range(3):
                piece(part, waits[0], i)[1]().wait_recv()
    if sends:
        for i in sends[1]:
            for part in range(3):
                piece(part, sends[0], i)[0]().start()
    if step == 5:
        for phase, count in ((2, 3), (1, 4), (0, 4)):
            for i in range(count):
                for part in range(3):
                    piece(part, phase, i)[0]().wait_send()


def muon_kernel(grad, momentum, weight, new_momentum, new_weight, weight_bf16, mine, other, acc, half, xm, xo, gram, poly, part_gram, full, stage, *scratch):
    ring = scratch[:12]
    load_sem, pair_ssem, pair_rsem, rs_ssem, rs_rsem, ag_ssem, ag_rsem, fw_ssem, fw_rsem, wg_ssem, wg_rsem, xc_ssem, xc_rsem, out_sem, po_ssem, po_rsem = scratch[12:]
    place = Place()
    z, y, x = place.xyz
    stages = (2, 1, -1, 0)
    loads, swaps = {}, {}
    for s, by in enumerate(stages):
        for p, (first, width, order) in enumerate(PARTS):
            axis = order[0]
            bz, bly, bx, r, c = at({axis: place.shifted(axis, by)}, ALL, pl.ds(first, width))
            loads[p, by] = pltpu.make_async_copy(grad.at[bz, bly, bx, place.core, r, c], acc.at[bz, bly, bx, r, c], load_sem.at[p, s])
            loads[p, by].start()
    greet(place)
    for s, by in enumerate(stages):
        for p, (first, width, order) in enumerate(PARTS):
            axis = order[0]
            bz, bly, bx, r, c = at({axis: place.shifted(axis, by)}, ALL, pl.ds(first, width))
            swaps[p, by] = send(grad.at[bz, bly, bx, 1 - place.core, r, c], half.at[bz, bly, bx, r, c], pair_ssem.at[p, s], pair_rsem.at[p, s], place.partner())
    full[z, y, x] = weight[...]
    wstep = lambda i: weight_step(place, weight, full, wg_ssem, wg_rsem, i)
    wstep(0)

    def ready(part):
        def chunk_ready(by):
            first, width, order = PARTS[part]
            here = at({order[0]: place.shifted(order[0], by)}, ALL, pl.ds(first, width))
            loads[part, by].wait()
            swaps[part, by].wait_recv()
            acc[here] += half[here]
        return chunk_ready

    sent = list(swaps.values())
    for phase in range(3):
        sent += run_together([reduce_phase(place, acc, ring[4 * phase:4 * phase + 4], rs_ssem, rs_rsem, p, phase, ready(p) if phase == 0 else (lambda by: None)) for p in range(3)])

    g = acc[z, y, x] / GROUP
    mom = MOMENTUM * momentum[...] + g
    new_momentum[...] = mom
    mine[z, y, x] = (g + MOMENTUM * mom).astype(jnp.bfloat16)

    forwards = []

    def forward(part):
        def on_piece(i, where):
            forwards.append(send(mine.at[where], other.at[where], fw_ssem.at[part, i], fw_rsem.at[part, i], place.partner()))
        return on_piece

    for phase in (2, 1, 0):
        sent += run_together([gather_phase(place, mine, ag_ssem, ag_rsem, p, phase, forward(p) if phase == 0 else (lambda i, w: None)) for p in range(3)])
    wstep(1)
    for copy in forwards:
        copy.wait_recv()
    for copy in sent + forwards:
        copy.wait_send()

    total = jnp.zeros((8, COLS), jnp.float32)
    for buf in (mine, other):
        for i in range(RING):
            block = buf[i].reshape(BLK // 8, 8, COLS).astype(jnp.float32)
            total += jnp.sum(block * block, axis=0)
    norm = jnp.sqrt(jnp.sum(jnp.sum(total, axis=0, keepdims=True), axis=1, keepdims=True))
    inverse = 1.0 / (norm + 1e-7)
    for buf, dst in ((mine, xm), (other, xo)):
        for i in range(RING):
            block = (buf[i].reshape(BLK, COLS).astype(jnp.float32) * inverse).astype(jnp.bfloat16)
            dst[0, :, i * BLK:(i + 1) * BLK] = block.T

    def exchange(slot, n):
        cols = pl.ds(n * BLK, BLK)
        return pltpu.make_async_remote_copy(src_ref=xm.at[slot, :, cols], dst_ref=xo.at[slot, :, cols], send_sem=xc_ssem.at[slot, n], recv_sem=xc_rsem.at[slot, n], device_id=place.partner(), device_id_type=MESH)

    def mirror(dst, j, tall):
        dst[j * BLK:, j * BLK:(j + 1) * BLK] = tall
        if j < NBLK - 1:
            dst[j * BLK:(j + 1) * BLK, (j + 1) * BLK:] = tall[BLK:].T

    def newton_schulz(t, carry):
        now = lax.rem(t, 2)
        before = 1 - now
        for when, step in ((0, 2), (1, 3), (3, 4)):
            @pl.when(t == when)
            def _():
                wstep(step)

        @pl.when(t > 0)
        def _():
            for n in range(NBLK):
                cols = slice(n * BLK, (n + 1) * BLK)
                old = xm[before, :, cols]
                xm[now, :, cols] = (COEF_A * old.astype(jnp.float32) + dot(poly[...], old)).astype(jnp.bfloat16)
                exchange(now, n).start()

        for j in range(NBLK):
            rows = slice(j * BLK, COLS)
            part_gram[rows, j * BLK:(j + 1) * BLK] = lax.dot_general(xm[now, rows], xm[now, j * BLK:(j + 1) * BLK], NT, preferred_element_type=jnp.float32)

        @pl.when(t > 0)
        def _():
            for n in range(NBLK):
                exchange(now, n).wait()

        for j in range(NBLK):
            rows, cols = slice(j * BLK, COLS), slice(j * BLK, (j + 1) * BLK)
            tall = part_gram[rows, cols] + lax.dot_general(xo[now, rows], xo[now, cols], NT, preferred_element_type=jnp.float32)
            mirror(gram, j, tall.astype(jnp.bfloat16))
        for j in range(NBLK):
            rows, cols = slice(j * BLK, COLS), slice(j * BLK, (j + 1) * BLK)
            tall = COEF_B * gram[rows, cols].astype(jnp.float32) + COEF_C * dot(gram[rows, :], gram[:, cols])
            mirror(poly, j, tall.astype(jnp.bfloat16))
        return carry

    lax.fori_loop(0, NS_STEPS, newton_schulz, 0)
    wstep(5)
    last = (NS_STEPS - 1) % 2
    scale = 0.2 * math.sqrt(ROWS)
    outs = []
    for n in range(NBLK):
        cols = slice(n * BLK, (n + 1) * BLK)
        old = xm[last, :, cols]
        ortho = (COEF_A * old.astype(jnp.float32) + dot(poly[...], old)).astype(jnp.bfloat16)
        w = full[n]
        w = w - LEARN_RATE * (scale * ortho.T.astype(jnp.float32).reshape(w.shape) + WEIGHT_DECAY * w)
        full[n] = w
        stage[n] = w.astype(jnp.bfloat16)
        there = weight_bf16.at[n, :, :, place.core]
        outs.append(pltpu.make_async_copy(stage.at[n], there, out_sem.at[n]))
        outs[-1].start()
        outs.append(send(stage.at[n], there, po_ssem.at[n], po_rsem.at[n], place.partner()))
    new_weight[...] = full[z, y, x]
    for copy in outs:
        copy.wait()


def muon(grad, momentum, weight):
    ring = []
    for lead in ((RING, RING), (RING,), ()):
        ring += [pltpu.VMEM(lead + (SLAB, COLS), jnp.float32)] * 2 + [pltpu.VMEM(lead + (8, COLS), jnp.float32)] * 2
    dma = pltpu.SemaphoreType.DMA
    cube = (RING, RING, RING, SLAB, COLS)
    vmem = pl.BlockSpec(memory_space=pltpu.VMEM)
    anywhere = pl.BlockSpec(memory_space=pl.ANY)
    f32, bf16 = jnp.float32, jnp.bfloat16
    return pl.pallas_call(
        muon_kernel,
        out_shape=(jax.ShapeDtypeStruct((SLAB, COLS), f32), jax.ShapeDtypeStruct((SLAB, COLS), f32), jax.ShapeDtypeStruct((RING, RING, RING, 2, SLAB, COLS), bf16)),
        in_specs=[anywhere, vmem, vmem],
        out_specs=(vmem, vmem, anywhere),
        scratch_shapes=[pltpu.VMEM(cube, bf16), pltpu.VMEM(cube, bf16), pltpu.VMEM(cube, f32), pltpu.VMEM(cube, f32),
                        pltpu.VMEM((2, COLS, COLS), bf16), pltpu.VMEM((2, COLS, COLS), bf16), pltpu.VMEM((COLS, COLS), bf16), pltpu.VMEM((COLS, COLS), bf16),
                        pltpu.VMEM((COLS, COLS), f32), pltpu.VMEM(cube, f32), pltpu.VMEM(cube, bf16), *ring,
                        dma((3, 4)), dma((3, 4)), dma((3, 4)), dma((3, 3, 6)), dma((3, 3, 6)), dma((3, 3, 4)), dma((3, 3, 4)), dma((3, 5)), dma((3, 5)),
                        dma((3, 3, 4)), dma((3, 3, 4)), dma((2, NBLK)), dma((2, NBLK)), dma((NBLK,)), dma((NBLK,)), dma((NBLK,))],
        compiler_params=pltpu.CompilerParams(collective_id=0, has_side_effects=True, vmem_limit_bytes=62 << 20),
        name='muon',
    )(grad, momentum, weight)


def solution(mesh):
    def local_step(grad_part, momentum, weight):
        grad = grad_part.reshape(RING, RING, RING, 2, SLAB, COLS)
        new_momentum, new_weight, weight_bf16 = muon(grad, momentum[0], weight[0])
        return new_momentum[None], new_weight[None], weight_bf16.reshape(1, ROWS, COLS)

    return jax.shard_map(local_step, mesh=mesh, in_specs=(P(('mp', 'dp')), P('mp', 'dp'), P('mp', 'dp')), out_specs=(P('mp', 'dp'), P('mp', 'dp'), P('mp')), check_vma=False)
```

```python
import math
import jax
import jax.numpy as jnp
from jax import lax
from jax.experimental import pallas as pl
from jax.experimental.pallas import tpu as pltpu
from jax.sharding import PartitionSpec as P

MOMENTUM = 0.95
LEARN_RATE = 2.0
WEIGHT_DECAY = 0.25
NS_STEPS = 5
COEF_A = 3.4445
COEF_B = -4.7750
COEF_C = 2.0315

MESH = pl.DeviceIdType.MESH
RING = 4
CHIPS = 64
GROUP = 128
SLAB = 16
COLS = 1024
ROWS = 2048
Z, Y, X = 0, 1, 2
PARTS = ((0, 384, (X, Y, Z)), (384, 384, (Y, Z, X)), (768, 256, (Z, X, Y)))


class Place:
    def __init__(self):
        me = lax.axis_index('dp')
        self.core = lax.rem(me, 2)
        chip = lax.div(me, 2)
        self.xyz = (lax.div(chip, 16), lax.rem(lax.div(chip, 4), 4), lax.rem(chip, 4))

    def index(self, xyz, core):
        return ((xyz[0] * RING + xyz[1]) * RING + xyz[2]) * 2 + core

    def shifted(self, axis, by):
        return lax.rem(self.xyz[axis] + (by % RING), RING)

    def neighbour(self, axis, by):
        xyz = list(self.xyz)
        xyz[axis] = self.shifted(axis, by)
        return {'dp': self.index(xyz, self.core)}

    def partner(self):
        return {'dp': self.index(self.xyz, 1 - self.core)}


def greet(place):
    barrier = pltpu.get_barrier_semaphore()
    peers = [place.partner()] + [place.neighbour(a, s) for a in (Z, Y, X) for s in (1, -1, 2)]
    for peer in peers:
        pl.semaphore_signal(barrier, inc=1, device_id=peer, device_id_type=MESH)
    pl.semaphore_wait(barrier, len(peers))


def at(fixed, rows, cols):
    return tuple(fixed.get(a, slice(None)) for a in (Z, Y, X)) + (rows, cols)


def send(src, dst, ssem, rsem, peer):
    copy = pltpu.make_async_remote_copy(src_ref=src, dst_ref=dst, send_sem=ssem, recv_sem=rsem, device_id=peer, device_id_type=MESH)
    copy.start()
    return copy


ALL = slice(None)
LOW, HIGH = pl.ds(0, 8), pl.ds(8, 8)


def reduce_phase(place, acc, ring_refs, ssem, rsem, part, phase, ready):
    first, width, order = PARTS[part]
    axis = order[phase]
    cols = pl.ds(first, width)
    near_l, near_r, far_l, far_r = ring_refs
    fixed = {a: place.xyz[a] for a in order[:phase]}
    right, left = place.neighbour(axis, 1), place.neighbour(axis, -1)

    def chunk(by, rows):
        return at({**fixed, axis: place.shifted(axis, by)}, rows, cols)

    across = place.neighbour(axis, 2)

    def sub(rows):
        return tuple(ALL for _ in range(2 - phase)) + (rows, cols)

    started = []
    sems = lambda i: (ssem.at[part, phase, i], rsem.at[part, phase, i])
    if phase == 2:
        for i, (by, dst, peer) in enumerate(((2, far_l, across), (1, near_l, right), (-1, near_r, left))):
            started.append(send(acc.at[chunk(by, ALL)], dst.at[sub(ALL)], *sems(i), peer))
            yield
        for copy in started:
            copy.wait_recv()
        acc[chunk(0, ALL)] += near_l[sub(ALL)] + near_r[sub(ALL)] + far_l[sub(ALL)]
        return started
    ready(2)
    started.append(send(acc.at[chunk(2, LOW)], far_l.at[sub(ALL)], *sems(0), right))
    started.append(send(acc.at[chunk(2, HIGH)], far_r.at[sub(ALL)], *sems(1), left))
    yield
    ready(1)
    started.append(send(acc.at[chunk(1, HIGH)], near_l.at[sub(HIGH)], *sems(2), right))
    yield
    ready(-1)
    started.append(send(acc.at[chunk(-1, LOW)], near_r.at[sub(LOW)], *sems(3), left))
    yield
    started[0].wait_recv()
    acc[chunk(1, LOW)] += far_l[sub(ALL)]
    started.append(send(acc.at[chunk(1, LOW)], near_l.at[sub(LOW)], *sems(4), right))
    yield
    started[1].wait_recv()
    acc[chunk(-1, HIGH)] += far_r[sub(ALL)]
    started.append(send(acc.at[chunk(-1, HIGH)], near_r.at[sub(HIGH)], *sems(5), left))
    yield
    ready(0)
    yield
    for i in (2, 3, 4, 5):
        started[i].wait_recv()
    acc[chunk(0, ALL)] += near_l[sub(ALL)] + near_r[sub(ALL)]
    return started


def gather_phase(place, buf, ssem, rsem, part, phase, on_piece):
    first, width, order = PARTS[part]
    axis = order[phase]
    cols = pl.ds(first, width)
    fixed = {a: place.xyz[a] for a in order[:phase]}
    right, left, across = place.neighbour(axis, 1), place.neighbour(axis, -1), place.neighbour(axis, 2)
    free = [a for a in (Z, Y, X) if a in order[phase + 1:]]
    sems = lambda i: (ssem.at[part, phase, i], rsem.at[part, phase, i])

    def chunk(by, half=None):
        where = {**fixed, axis: place.shifted(axis, by)}
        if half is not None:
            where[free[0]] = pl.ds(2 * half, 2)
        return at(where, ALL, cols)

    def recv(i, by, half=None):
        there = buf.at[chunk(by, half)]
        pltpu.make_async_remote_copy(src_ref=there, dst_ref=there, send_sem=ssem.at[part, phase, i], recv_sem=rsem.at[part, phase, i], device_id=right, device_id_type=MESH).wait_recv()

    started = []
    if not free:
        mine = buf.at[chunk(0)]
        for i, peer in enumerate((across, right, left)):
            started.append(send(mine, mine, *sems(i), peer))
        yield
        recv(1, -1)
        recv(2, 1)
        recv(0, 2)
        return started
    for i, half, peer in ((0, 0, right), (1, 1, left), (2, 1, right), (3, 0, left)):
        mine = buf.at[chunk(0, half)]
        started.append(send(mine, mine, *sems(i), peer))
    on_piece(0, chunk(0))
    yield
    recv(0, -1, 0)
    there = buf.at[chunk(-1, 0)]
    started.append(send(there, there, *sems(4), right))
    on_piece(1, chunk(-1, 0))
    yield
    recv(1, 1, 1)
    there = buf.at[chunk(1, 1)]
    started.append(send(there, there, *sems(5), left))
    on_piece(2, chunk(1, 1))
    yield
    for i, by, half in ((2, -1, 1), (3, 1, 0), (4, 2, 0), (5, 2, 1)):
        recv(i, by, half)
        on_piece(i + 1, chunk(by, half))
        yield
    return started


def run_together(generators):
    started, live = [], list(generators)
    while live:
        left = []
        for g in live:
            try:
                next(g)
                left.append(g)
            except StopIteration as stop:
                started.extend(stop.value)
        live = left
    return started


NT = (((1,), (1,)), ((), ()))
BLK = 256
NBLK = COLS // BLK


WIDE = 512


def dot_nt(a, b):
    return lax.dot_general(a, b, NT, preferred_element_type=jnp.float32)


def square(n):
    return slice((n % 2) * WIDE, (n % 2 + 1) * WIDE), slice((n // 2) * WIDE, (n // 2 + 1) * WIDE)


def dot(a, b):
    return jnp.dot(a, b, preferred_element_type=jnp.float32)


def weight_step(place, weight, full, ssem, rsem, step):
    def piece(part, phase, i):
        first, width, order = PARTS[part]
        axis = order[phase]
        cols = pl.ds(first, width)
        fixed = {a: place.xyz[a] for a in order[:phase]}
        free = [a for a in (Z, Y, X) if a in order[phase + 1:]]
        right, left, across = place.neighbour(axis, 1), place.neighbour(axis, -1), place.neighbour(axis, 2)

        def chunk(by, half=None):
            where = {**fixed, axis: place.shifted(axis, by)}
            if half is not None:
                where[free[0]] = pl.ds(2 * half, 2)
            return full.at[at(where, ALL, cols)]

        if not free:
            src_by, half, peer, from_by = ((0, None, right, -1), (0, None, left, 1), (0, None, across, 2))[i]
        else:
            src_by, half, peer, from_by = ((0, None, right, -1), (0, None, left, 1), (-1, 0, right, 2), (1, 1, left, 2))[i]
        out = chunk(src_by, half)
        src = weight.at[:, cols] if not free else out
        go = lambda: pltpu.make_async_remote_copy(src_ref=src, dst_ref=out, send_sem=ssem.at[part, phase, i], recv_sem=rsem.at[part, phase, i], device_id=peer, device_id_type=MESH)
        came = chunk(from_by, half)
        come = lambda: pltpu.make_async_remote_copy(src_ref=came, dst_ref=came, send_sem=ssem.at[part, phase, i], recv_sem=rsem.at[part, phase, i], device_id=peer, device_id_type=MESH)
        return go, come

    plan = {0: ((), (2, (0, 1, 2))), 1: ((2, (0, 1, 2)), (1, (0, 1))), 2: ((1, (0, 1)), (1, (2, 3))), 3: ((1, (2, 3)), (0, (0, 1))), 4: ((0, (0, 1)), (0, (2, 3))), 5: ((0, (2, 3)), ())}
    waits, sends = plan[step]
    if waits:
        for i in waits[1]:
            for part in range(3):
                piece(part, waits[0], i)[1]().wait_recv()
    if sends:
        for i in sends[1]:
            for part in range(3):
                piece(part, sends[0], i)[0]().start()
    if step == 5:
        for phase, count in ((2, 3), (1, 4), (0, 4)):
            for i in range(count):
                for part in range(3):
                    piece(part, phase, i)[0]().wait_send()


def muon_kernel(grad, momentum, weight, new_momentum, new_weight, weight_bf16, mine, other, acc, half, xm, xo, gram, poly, part_gram, full, old_mom, old_weight, *scratch):
    ring = scratch[:12]
    load_sem, pair_ssem, pair_rsem, rs_ssem, rs_rsem, ag_ssem, ag_rsem, fw_ssem, fw_rsem, wg_ssem, wg_rsem, xc_ssem, xc_rsem, po_ssem, po_rsem, in_sem = scratch[12:]
    place = Place()
    z, y, x = place.xyz
    stages = (2, 1, -1, 0)
    loads, swaps = {}, {}
    for s, by in enumerate(stages):
        for p, (first, width, order) in enumerate(PARTS):
            axis = order[0]
            bz, bly, bx, r, c = at({axis: place.shifted(axis, by)}, ALL, pl.ds(first, width))
            loads[p, by] = pltpu.make_async_copy(grad.at[bz, bly, bx, place.core, r, c], acc.at[bz, bly, bx, r, c], load_sem.at[p, s])
            loads[p, by].start()
    into = (pltpu.make_async_copy(momentum, old_mom, in_sem.at[0]), pltpu.make_async_copy(weight, old_weight, in_sem.at[1]))
    for copy in into:
        copy.start()
    greet(place)
    for s, by in enumerate(stages):
        for p, (first, width, order) in enumerate(PARTS):
            axis = order[0]
            bz, bly, bx, r, c = at({axis: place.shifted(axis, by)}, ALL, pl.ds(first, width))
            swaps[p, by] = send(grad.at[bz, bly, bx, 1 - place.core, r, c], half.at[bz, bly, bx, r, c], pair_ssem.at[p, s], pair_rsem.at[p, s], place.partner())
    for copy in into:
        copy.wait()
    full[z, y, x] = old_weight[...]
    wstep = lambda i: weight_step(place, old_weight, full, wg_ssem, wg_rsem, i)
    wstep(0)

    def ready(part):
        def chunk_ready(by):
            first, width, order = PARTS[part]
            here = at({order[0]: place.shifted(order[0], by)}, ALL, pl.ds(first, width))
            loads[part, by].wait()
            swaps[part, by].wait_recv()
            acc[here] += half[here]
        return chunk_ready

    sent = list(swaps.values())
    for phase in range(3):
        sent += run_together([reduce_phase(place, acc, ring[4 * phase:4 * phase + 4], rs_ssem, rs_rsem, p, phase, ready(p) if phase == 0 else (lambda by: None)) for p in range(3)])

    g = acc[z, y, x] / GROUP
    mom = MOMENTUM * old_mom[...] + g
    new_momentum[...] = mom
    mine[z, y, x] = (g + MOMENTUM * mom).astype(jnp.bfloat16)

    forwards = []

    def forward(part):
        def on_piece(i, where):
            forwards.append(send(mine.at[where], other.at[where], fw_ssem.at[part, i], fw_rsem.at[part, i], place.partner()))
        return on_piece

    for phase in (2, 1, 0):
        sent += run_together([gather_phase(place, mine, ag_ssem, ag_rsem, p, phase, forward(p) if phase == 0 else (lambda i, w: None)) for p in range(3)])
    wstep(1)
    for copy in forwards:
        copy.wait_recv()
    for copy in sent + forwards:
        copy.wait_send()

    total = jnp.zeros((8, COLS), jnp.float32)
    for buf in (mine, other):
        for i in range(RING):
            block = buf[i].reshape(BLK // 8, 8, COLS).astype(jnp.float32)
            total += jnp.sum(block * block, axis=0)
    norm = jnp.sqrt(jnp.sum(jnp.sum(total, axis=0, keepdims=True), axis=1, keepdims=True))
    inverse = 1.0 / (norm + 1e-7)
    for buf, dst in ((mine, xm), (other, xo)):
        for i in range(RING):
            block = (buf[i].reshape(BLK, COLS).astype(jnp.float32) * inverse).astype(jnp.bfloat16)
            dst[0, :, i * BLK:(i + 1) * BLK] = block.T

    def exchange(slot, n):
        rows, cols = square(n)
        return pltpu.make_async_remote_copy(src_ref=xm.at[slot, rows, cols], dst_ref=xo.at[slot, rows, cols], send_sem=xc_ssem.at[slot, n], recv_sem=xc_rsem.at[slot, n], device_id=place.partner(), device_id_type=MESH)

    def mirror(dst, j, tall):
        dst[j * BLK:, j * BLK:(j + 1) * BLK] = tall
        if j < NBLK - 1:
            dst[j * BLK:(j + 1) * BLK, (j + 1) * BLK:] = tall[BLK:].T

    def newton_schulz(t, carry):
        now = lax.rem(t, 2)
        before = 1 - now
        for when, step in ((0, 2), (1, 3), (3, 4)):
            @pl.when(t == when)
            def _():
                wstep(step)

        @pl.when(t > 0)
        def _():
            for n in range(4):
                rows, cols = square(n)
                old = xm[before, :, cols]
                xm[now, rows, cols] = (COEF_A * xm[before, rows, cols].astype(jnp.float32) + dot(poly[rows, :], old)).astype(jnp.bfloat16)
                exchange(now, n).start()

        for j in range(NBLK):
            rows = slice(j * BLK, COLS)
            part_gram[rows, j * BLK:(j + 1) * BLK] = dot_nt(xm[now, rows], xm[now, j * BLK:(j + 1) * BLK])

        for k in range(2):
            @pl.when(t > 0)
            def _():
                for n in (2 * k, 2 * k + 1):
                    exchange(now, n).wait()

            deep = slice(k * WIDE, (k + 1) * WIDE)
            for j in range(NBLK):
                rows, cols = slice(j * BLK, COLS), slice(j * BLK, (j + 1) * BLK)
                tall = part_gram[rows, cols] + dot_nt(xo[now, rows, deep], xo[now, cols, deep])
                if k == 0:
                    part_gram[rows, cols] = tall
                else:
                    mirror(gram, j, tall.astype(jnp.bfloat16))
        for j in range(NBLK):
            rows, cols = slice(j * BLK, COLS), slice(j * BLK, (j + 1) * BLK)
            tall = COEF_B * gram[rows, cols].astype(jnp.float32) + COEF_C * dot_nt(gram[rows, :], gram[cols, :])
            mirror(poly, j, tall.astype(jnp.bfloat16))
        return carry

    lax.fori_loop(0, NS_STEPS, newton_schulz, 0)
    wstep(5)
    last = (NS_STEPS - 1) % 2
    scale = 0.2 * math.sqrt(ROWS)
    outs = []
    for n in range(NBLK):
        if n % 2 == 0:
            cols = slice(n * BLK, n * BLK + WIDE)
            old = xm[last, :, cols]
            wide = (COEF_A * old.astype(jnp.float32) + dot(poly[...], old)).astype(jnp.bfloat16)
        ortho = wide[:, (n % 2) * BLK:(n % 2 + 1) * BLK]
        w = full[n]
        w = w - LEARN_RATE * (scale * ortho.T.astype(jnp.float32).reshape(w.shape) + WEIGHT_DECAY * w)
        full[n] = w
        weight_bf16[n, :, :, place.core] = w.astype(jnp.bfloat16)
        there = weight_bf16.at[n, :, :, place.core]
        outs.append(send(there, there, po_ssem.at[n], po_rsem.at[n], place.partner()))
    new_weight[...] = full[z, y, x]
    for copy in outs:
        copy.wait()


def muon(grad, momentum, weight):
    ring = []
    for lead in ((RING, RING), (RING,), ()):
        ring += [pltpu.VMEM(lead + (SLAB, COLS), jnp.float32)] * 2 + [pltpu.VMEM(lead + (8 if lead else SLAB, COLS), jnp.float32)] * 2
    dma = pltpu.SemaphoreType.DMA
    cube = (RING, RING, RING, SLAB, COLS)
    vmem = pl.BlockSpec(memory_space=pltpu.VMEM)
    hbm = pl.BlockSpec(memory_space=pltpu.HBM)
    anywhere = pl.BlockSpec(memory_space=pl.ANY)
    f32, bf16 = jnp.float32, jnp.bfloat16
    return pl.pallas_call(
        muon_kernel,
        out_shape=(jax.ShapeDtypeStruct((SLAB, COLS), f32), jax.ShapeDtypeStruct((SLAB, COLS), f32), jax.ShapeDtypeStruct((RING, RING, RING, 2, SLAB, COLS), bf16)),
        in_specs=[anywhere, hbm, hbm],
        out_specs=(vmem, vmem, vmem),
        scratch_shapes=[pltpu.VMEM(cube, bf16), pltpu.VMEM(cube, bf16), pltpu.VMEM(cube, f32), pltpu.VMEM(cube, f32),
                        pltpu.VMEM((2, COLS, COLS), bf16), pltpu.VMEM((2, COLS, COLS), bf16), pltpu.VMEM((COLS, COLS), bf16), pltpu.VMEM((COLS, COLS), bf16),
                        pltpu.VMEM((COLS, COLS), f32), pltpu.VMEM(cube, f32), pltpu.VMEM((SLAB, COLS), f32), pltpu.VMEM((SLAB, COLS), f32), *ring,
                        dma((3, 4)), dma((3, 4)), dma((3, 4)), dma((3, 3, 6)), dma((3, 3, 6)), dma((3, 3, 6)), dma((3, 3, 6)), dma((3, 7)), dma((3, 7)),
                        dma((3, 3, 4)), dma((3, 3, 4)), dma((2, NBLK)), dma((2, NBLK)), dma((NBLK,)), dma((NBLK,)), dma((2,))],
        compiler_params=pltpu.CompilerParams(collective_id=0, has_side_effects=True, vmem_limit_bytes=46 << 20),
        name='muon',
    )(grad, momentum, weight)


def put_kernel(*refs):
    sems = refs[-1]
    copies = [pltpu.make_async_copy(refs[i], refs[3 + i], sems.at[i]) for i in (2, 1, 0)]
    for copy in copies:
        copy.start()
    for copy in copies:
        copy.wait()


def put(*values):
    return pl.pallas_call(
        put_kernel,
        out_shape=tuple(jax.ShapeDtypeStruct(v.shape, v.dtype) for v in values),
        in_specs=[pl.BlockSpec(memory_space=pltpu.VMEM)] * 3,
        out_specs=(pl.BlockSpec(memory_space=pltpu.HBM),) * 3,
        scratch_shapes=[pltpu.SemaphoreType.DMA((3,))],
        compiler_params=pltpu.CompilerParams(vmem_limit_bytes=8 << 20),
        name='put',
    )(*values)


def solution(mesh):
    def local_step(grad_part, momentum, weight):
        grad = grad_part.reshape(RING, RING, RING, 2, SLAB, COLS)
        new_momentum, new_weight, weight_bf16 = put(*muon(grad, *(pltpu.with_memory_space_constraint(v[0], pltpu.HBM) for v in (momentum, weight))))
        return new_momentum[None], new_weight[None], weight_bf16.reshape(1, ROWS, COLS)

    return jax.shard_map(local_step, mesh=mesh, in_specs=(P(('mp', 'dp')), P('mp', 'dp'), P('mp', 'dp')), out_specs=(P('mp', 'dp'), P('mp', 'dp'), P('mp')), check_vma=False)
```

```python
import math
import jax
import jax.numpy as jnp
from jax import lax
from jax.experimental import pallas as pl
from jax.experimental.pallas import tpu as pltpu
from jax.sharding import PartitionSpec as P

MOMENTUM = 0.95
LEARN_RATE = 2.0
WEIGHT_DECAY = 0.25
NS_STEPS = 5
COEF_A = 3.4445
COEF_B = -4.7750
COEF_C = 2.0315

MESH = pl.DeviceIdType.MESH
RING = 4
CHIPS = 64
GROUP = 128
SLAB = 16
COLS = 1024
ROWS = 2048
Z, Y, X = 0, 1, 2
PARTS = ((0, 384, (X, Y, Z)), (384, 384, (Y, Z, X)), (768, 256, (Z, X, Y)))


class Place:
    def __init__(self):
        me = lax.axis_index('dp')
        self.core = lax.rem(me, 2)
        chip = lax.div(me, 2)
        self.xyz = (lax.div(chip, 16), lax.rem(lax.div(chip, 4), 4), lax.rem(chip, 4))

    def index(self, xyz, core):
        return ((xyz[0] * RING + xyz[1]) * RING + xyz[2]) * 2 + core

    def shifted(self, axis, by):
        return lax.rem(self.xyz[axis] + (by % RING), RING)

    def neighbour(self, axis, by):
        xyz = list(self.xyz)
        xyz[axis] = self.shifted(axis, by)
        return {'dp': self.index(xyz, self.core)}

    def partner(self):
        return {'dp': self.index(self.xyz, 1 - self.core)}


def greet(place):
    barrier = pltpu.get_barrier_semaphore()
    peers = [place.partner()] + [place.neighbour(a, s) for a in (Z, Y, X) for s in (1, -1, 2)]
    for peer in peers:
        pl.semaphore_signal(barrier, inc=1, device_id=peer, device_id_type=MESH)
    pl.semaphore_wait(barrier, len(peers))


def at(fixed, rows, cols):
    return tuple(fixed.get(a, slice(None)) for a in (Z, Y, X)) + (rows, cols)


def send(src, dst, ssem, rsem, peer):
    copy = pltpu.make_async_remote_copy(src_ref=src, dst_ref=dst, send_sem=ssem, recv_sem=rsem, device_id=peer, device_id_type=MESH)
    copy.start()
    return copy


ALL = slice(None)
BATCHES = 1
LEAD = SLAB // BATCHES
STEPS = ('far0', 'near0', 'far1', 'near1', 'near2', 'all2', 'half1', 'full1', 'half0', 'rest0', 'full0')
LAG = 0.5


class Line:
    def __init__(self, place, part, batch, phase):
        first, width, order = PARTS[part]
        self.place, self.axis = place, order[phase]
        self.rows, self.cols = pl.ds(LEAD * batch, LEAD), pl.ds(first, width)
        self.fixed = {a: place.xyz[a] for a in order[:phase]}
        self.free = [a for a in (Z, Y, X) if a in order[phase + 1:]]
        self.right, self.left, self.across = (place.neighbour(self.axis, by) for by in (1, -1, 2))

    def chunk(self, by, half=None):
        where = {**self.fixed, self.axis: self.place.shifted(self.axis, by)}
        if half is not None:
            where[self.free[0]] = pl.ds(2 * half, 2)
        return at(where, self.rows, self.cols)

    def slot(self, half=None):
        lead = [ALL] * len(self.free)
        if half is not None:
            lead[0] = pl.ds(2 * half, 2)
        return (*lead, self.rows, self.cols)


def reduce_chain(place, acc, ring, ssem, rsem, part, batch, ready, sent):
    for phase in range(3):
        line = Line(place, part, batch, phase)
        near_l, near_r, far_l, far_r = ring[4 * phase:4 * phase + 4]
        chunk, slot, right, left = line.chunk, line.slot, line.right, line.left

        def go(i, src, dst, peer):
            copy = send(src, dst, ssem.at[part, batch, phase, i], rsem.at[part, batch, phase, i], peer)
            sent.append(copy)
            return copy

        if phase == 2:
            copies = [go(0, acc.at[chunk(2)], far_l.at[slot()], line.across), go(1, acc.at[chunk(1)], near_l.at[slot()], right), go(2, acc.at[chunk(-1)], near_r.at[slot()], left)]
            yield 'near2'
            for copy in copies:
                copy.wait_recv()
            acc[chunk(0)] += near_l[slot()] + near_r[slot()] + far_l[slot()]
            continue
        if phase == 0:
            yield 'swap', 0
            ready(2)
        far = go(0, acc.at[chunk(2, 0)], far_l.at[slot()], right), go(1, acc.at[chunk(2, 1)], far_r.at[slot()], left)
        if phase == 0:
            yield 'swap', 1
            ready(1)
        near = [go(2, acc.at[chunk(1, 1)], near_l.at[slot(1)], right)]
        if phase == 0:
            yield 'swap', 2
            ready(-1)
        near.append(go(3, acc.at[chunk(-1, 0)], near_r.at[slot(0)], left))
        if phase == 0:
            yield 'swap', 3
            ready(0)
        yield 'far%d' % phase
        far[0].wait_recv()
        acc[chunk(1, 0)] += far_l[slot()]
        near.append(go(4, acc.at[chunk(1, 0)], near_l.at[slot(0)], right))
        yield 'far%d' % phase
        far[1].wait_recv()
        acc[chunk(-1, 1)] += far_r[slot()]
        near.append(go(5, acc.at[chunk(-1, 1)], near_r.at[slot(1)], left))
        yield 'near%d' % phase
        for copy in near:
            copy.wait_recv()
        acc[chunk(0)] += near_l[slot()] + near_r[slot()]


def gather_chain(place, buf, ssem, rsem, part, batch, on_piece, sent):
    for phase in (2, 1, 0):
        line = Line(place, part, batch, phase)
        chunk, right, left = line.chunk, line.right, line.left

        def go(i, where, peer):
            sent.append(send(buf.at[where], buf.at[where], ssem.at[part, batch, phase, i], rsem.at[part, batch, phase, i], peer))

        def recv(i, where):
            there = buf.at[where]
            pltpu.make_async_remote_copy(src_ref=there, dst_ref=there, send_sem=ssem.at[part, batch, phase, i], recv_sem=rsem.at[part, batch, phase, i], device_id=right, device_id_type=MESH).wait_recv()

        def piece(i, where):
            if phase == 0:
                on_piece(i, where)

        if phase == 2:
            for i, peer in enumerate((line.across, right, left)):
                go(i, chunk(0), peer)
            yield 'all2'
            recv(1, chunk(-1))
            recv(2, chunk(1))
            recv(0, chunk(2))
            continue
        for i, half, peer in ((0, 0, right), (1, 1, left), (2, 1, right), (3, 0, left)):
            go(i, chunk(0, half), peer)
        piece(0, chunk(0))
        yield 'half%d' % phase
        recv(0, chunk(-1, 0))
        go(4, chunk(-1, 0), right)
        piece(1, chunk(-1, 0))
        yield 'half%d' % phase
        recv(1, chunk(1, 1))
        go(5, chunk(1, 1), left)
        piece(2, chunk(1, 1))
        for i, by, half in ((2, -1, 1), (3, 1, 0), (4, 2, 0), (5, 2, 1)):
            if i == 2 or i == 4:
                yield 'full%d' % phase if i == 4 or phase == 1 else 'rest0'
            recv(i, chunk(by, half))
            piece(i + 1, chunk(by, half))


def run_chains(chains):
    queue = []

    def step(number, batch, chain):
        name = next(chain, None)
        if name is not None:
            due = batch - 9 + name[1] / 9 if isinstance(name, tuple) else STEPS.index(name) + LAG * batch
            queue.append((due, number, batch, chain))

    for number, (batch, chain) in enumerate(chains):
        step(number, batch, chain)
    while queue:
        queue.sort(key=lambda entry: entry[:2])
        step(*queue.pop(0)[1:])


NT = (((1,), (1,)), ((), ()))
BLK = 256
NBLK = COLS // BLK


WIDE = 512


def dot_nt(a, b):
    return lax.dot_general(a, b, NT, preferred_element_type=jnp.float32)


def square(n):
    return slice((n % 2) * WIDE, (n % 2 + 1) * WIDE), slice((n // 2) * WIDE, (n // 2 + 1) * WIDE)


def dot(a, b):
    return jnp.dot(a, b, preferred_element_type=jnp.float32)


def weight_step(place, weight, full, ssem, rsem, step):
    def piece(part, phase, i):
        first, width, order = PARTS[part]
        axis = order[phase]
        cols = pl.ds(first, width)
        fixed = {a: place.xyz[a] for a in order[:phase]}
        free = [a for a in (Z, Y, X) if a in order[phase + 1:]]
        right, left, across = place.neighbour(axis, 1), place.neighbour(axis, -1), place.neighbour(axis, 2)

        def chunk(by, half=None):
            where = {**fixed, axis: place.shifted(axis, by)}
            if half is not None:
                where[free[0]] = pl.ds(2 * half, 2)
            return full.at[at(where, ALL, cols)]

        if not free:
            src_by, half, peer, from_by = ((0, None, right, -1), (0, None, left, 1), (0, None, across, 2))[i]
        else:
            src_by, half, peer, from_by = ((0, None, right, -1), (0, None, left, 1), (-1, 0, right, 2), (1, 1, left, 2))[i]
        out = chunk(src_by, half)
        src = weight.at[:, cols] if not free else out
        go = lambda: pltpu.make_async_remote_copy(src_ref=src, dst_ref=out, send_sem=ssem.at[part, phase, i], recv_sem=rsem.at[part, phase, i], device_id=peer, device_id_type=MESH)
        came = chunk(from_by, half)
        come = lambda: pltpu.make_async_remote_copy(src_ref=came, dst_ref=came, send_sem=ssem.at[part, phase, i], recv_sem=rsem.at[part, phase, i], device_id=peer, device_id_type=MESH)
        return go, come

    plan = {0: ((), (2, (0, 1, 2))), 1: ((2, (0, 1, 2)), (1, (0, 1))), 2: ((1, (0, 1)), (1, (2, 3))), 3: ((1, (2, 3)), (0, (0, 1))), 4: ((0, (0, 1)), (0, (2, 3))), 5: ((0, (2, 3)), ())}
    waits, sends = plan[step]
    if waits:
        for i in waits[1]:
            for part in range(3):
                piece(part, waits[0], i)[1]().wait_recv()
    if sends:
        for i in sends[1]:
            for part in range(3):
                piece(part, sends[0], i)[0]().start()
    if step == 5:
        for phase, count in ((2, 3), (1, 4), (0, 4)):
            for i in range(count):
                for part in range(3):
                    piece(part, phase, i)[0]().wait_send()


def muon_kernel(grad, momentum, weight, new_momentum, new_weight, weight_bf16, mine, other, acc, half, xm, xo, gram, poly, part_gram, full, old_mom, old_weight, *scratch):
    ring = scratch[:12]
    load_sem, pair_ssem, pair_rsem, rs_ssem, rs_rsem, ag_ssem, ag_rsem, fw_ssem, fw_rsem, wg_ssem, wg_rsem, xc_ssem, xc_rsem, po_ssem, po_rsem, in_sem = scratch[12:]
    place = Place()
    z, y, x = place.xyz
    stages = (2, 1, -1, 0)
    order = [(b, s, p) for b in range(BATCHES) for s in range(4) for p in range(3)]
    loads, swaps, sent, forwards = {}, {}, [], []

    def block(b, s, p):
        axis = PARTS[p][2][0]
        return at({axis: place.shifted(axis, stages[s])}, pl.ds(LEAD * b, LEAD), pl.ds(*PARTS[p][:2]))

    for b, s, p in order:
        bz, by, bx, r, c = here = block(b, s, p)
        loads[p, b, stages[s]] = pltpu.make_async_copy(grad.at[bz, by, bx, place.core, r, c], acc.at[here], load_sem.at[p, b, s])
        loads[p, b, stages[s]].start()
    into = (pltpu.make_async_copy(momentum, old_mom, in_sem.at[0]), pltpu.make_async_copy(weight, old_weight, in_sem.at[1]))
    for copy in into:
        copy.start()
    greet(place)
    for b, s, p in order:
        bz, by, bx, r, c = here = block(b, s, p)
        swaps[p, b, stages[s]] = send(grad.at[bz, by, bx, 1 - place.core, r, c], half.at[here], pair_ssem.at[p, b, s], pair_rsem.at[p, b, s], place.partner())
    for copy in into:
        copy.wait()
    full[z, y, x] = old_weight[...]
    wstep = lambda i: weight_step(place, old_weight, full, wg_ssem, wg_rsem, i)
    wstep(0)

    def chain(p, b):
        cols, rows = pl.ds(*PARTS[p][:2]), pl.ds(LEAD * b, LEAD)

        def ready(by):
            here = block(b, stages.index(by), p)
            loads[p, b, by].wait()
            swaps[p, b, by].wait_recv()
            acc[here] += half[here]

        def forward(i, where):
            forwards.append(send(mine.at[where], other.at[where], fw_ssem.at[p, b, i], fw_rsem.at[p, b, i], place.partner()))

        yield from reduce_chain(place, acc, ring, rs_ssem, rs_rsem, p, b, ready, sent)
        g = acc[z, y, x, rows, cols] / GROUP
        mom = MOMENTUM * old_mom[rows, cols] + g
        new_momentum[rows, cols] = mom
        mine[z, y, x, rows, cols] = (g + MOMENTUM * mom).astype(jnp.bfloat16)
        yield from gather_chain(place, mine, ag_ssem, ag_rsem, p, b, forward, sent)

    run_chains([(b, chain(p, b)) for b in range(BATCHES) for p in range(3)])
    wstep(1)

    def squares(buf, total):
        for i in range(RING):
            block = buf[i].reshape(BLK // 8, 8, COLS).astype(jnp.float32)
            total += jnp.sum(block * block, axis=0)
        return total

    total = squares(mine, jnp.zeros((8, COLS), jnp.float32))
    for copy in forwards:
        copy.wait_recv()
    total = squares(other, total)
    for copy in sent + forwards + list(swaps.values()):
        copy.wait_send()
    norm = jnp.sqrt(jnp.sum(jnp.sum(total, axis=0, keepdims=True), axis=1, keepdims=True))
    inverse = 1.0 / (norm + 1e-7)
    for buf, dst in ((mine, xm), (other, xo)):
        for i in range(RING):
            block = (buf[i].reshape(BLK, COLS).astype(jnp.float32) * inverse).astype(jnp.bfloat16)
            dst[0, :, i * BLK:(i + 1) * BLK] = block.T

    def exchange(slot, n):
        rows, cols = square(n)
        return pltpu.make_async_remote_copy(src_ref=xm.at[slot, rows, cols], dst_ref=xo.at[slot, rows, cols], send_sem=xc_ssem.at[slot, n], recv_sem=xc_rsem.at[slot, n], device_id=place.partner(), device_id_type=MESH)

    def mirror(dst, j, tall):
        dst[j * BLK:, j * BLK:(j + 1) * BLK] = tall
        if j < NBLK - 1:
            dst[j * BLK:(j + 1) * BLK, (j + 1) * BLK:] = tall[BLK:].T

    def newton_schulz(t, carry):
        now = lax.rem(t, 2)
        before = 1 - now
        @pl.when(t > 0)
        def _():
            for k in range(2):
                cols = slice(k * WIDE, (k + 1) * WIDE)
                old = xm[before, :, cols]
                xm[now, :, cols] = (COEF_A * old.astype(jnp.float32) + dot(poly[...], old)).astype(jnp.bfloat16)
                exchange(now, 2 * k).start()
                exchange(now, 2 * k + 1).start()

        for j in range(NBLK):
            rows = slice(j * BLK, COLS)
            part_gram[rows, j * BLK:(j + 1) * BLK] = dot_nt(xm[now, rows], xm[now, j * BLK:(j + 1) * BLK])

        for k in range(2):
            @pl.when(t > 0)
            def _():
                for n in (2 * k, 2 * k + 1):
                    exchange(now, n).wait()

            deep = slice(k * WIDE, (k + 1) * WIDE)
            for j in range(NBLK):
                rows, cols = slice(j * BLK, COLS), slice(j * BLK, (j + 1) * BLK)
                tall = part_gram[rows, cols] + dot_nt(xo[now, rows, deep], xo[now, cols, deep])
                if k == 0:
                    part_gram[rows, cols] = tall
                else:
                    mirror(gram, j, tall.astype(jnp.bfloat16))
        for j in range(NBLK):
            rows, cols = slice(j * BLK, COLS), slice(j * BLK, (j + 1) * BLK)
            tall = COEF_B * gram[rows, cols].astype(jnp.float32) + COEF_C * dot_nt(gram[rows, :], gram[cols, :])
            mirror(poly, j, tall.astype(jnp.bfloat16))

        for when, step in ((0, 2), (1, 3), (3, 4)):
            @pl.when(t == when)
            def _():
                wstep(step)
        return carry

    lax.fori_loop(0, NS_STEPS, newton_schulz, 0)
    last = (NS_STEPS - 1) % 2
    scale = 0.2 * math.sqrt(ROWS)
    outs = []
    for n in range(NBLK):
        if n % 2 == 0:
            cols = slice(n * BLK, n * BLK + WIDE)
            old = xm[last, :, cols]
            pair = (COEF_A * old.astype(jnp.float32) + dot(poly[...], old)).astype(jnp.bfloat16)
        if n == 0:
            wstep(5)
        ortho = pair[:, (n % 2) * BLK:(n % 2 + 1) * BLK]
        w = full[n]
        w = w - LEARN_RATE * (scale * ortho.T.astype(jnp.float32).reshape(w.shape) + WEIGHT_DECAY * w)
        full[n] = w
        weight_bf16[n, :, :, place.core] = w.astype(jnp.bfloat16)
        there = weight_bf16.at[n, :, :, place.core]
        outs.append(send(there, there, po_ssem.at[n], po_rsem.at[n], place.partner()))
    new_weight[...] = full[z, y, x]
    for copy in outs:
        copy.wait()


def muon(grad, momentum, weight):
    ring = []
    for lead, split in (((RING, RING), (2, RING)), ((RING,), (2,)), ((), ())):
        ring += [pltpu.VMEM(lead + (SLAB, COLS), jnp.float32)] * 2 + [pltpu.VMEM(split + (SLAB, COLS), jnp.float32)] * 2
    dma = pltpu.SemaphoreType.DMA
    cube = (RING, RING, RING, SLAB, COLS)
    vmem = pl.BlockSpec(memory_space=pltpu.VMEM)
    hbm = pl.BlockSpec(memory_space=pltpu.HBM)
    anywhere = pl.BlockSpec(memory_space=pl.ANY)
    f32, bf16 = jnp.float32, jnp.bfloat16
    return pl.pallas_call(
        muon_kernel,
        out_shape=(jax.ShapeDtypeStruct((SLAB, COLS), f32), jax.ShapeDtypeStruct((SLAB, COLS), f32), jax.ShapeDtypeStruct((RING, RING, RING, 2, SLAB, COLS), bf16)),
        in_specs=[anywhere, hbm, hbm],
        out_specs=(vmem, vmem, vmem),
        scratch_shapes=[pltpu.VMEM(cube, bf16), pltpu.VMEM(cube, bf16), pltpu.VMEM(cube, f32), pltpu.VMEM(cube, f32),
                        pltpu.VMEM((2, COLS, COLS), bf16), pltpu.VMEM((2, COLS, COLS), bf16), pltpu.VMEM((COLS, COLS), bf16), pltpu.VMEM((COLS, COLS), bf16),
                        pltpu.VMEM((COLS, COLS), f32), pltpu.VMEM(cube, f32), pltpu.VMEM((SLAB, COLS), f32), pltpu.VMEM((SLAB, COLS), f32), *ring,
                        *[dma((3, BATCHES, 4))] * 3, *[dma((3, BATCHES, 3, 6))] * 4, *[dma((3, BATCHES, 7))] * 2,
                        dma((3, 3, 4)), dma((3, 3, 4)), dma((2, NBLK)), dma((2, NBLK)), dma((NBLK,)), dma((NBLK,)), dma((2,))],
        compiler_params=pltpu.CompilerParams(collective_id=0, has_side_effects=True, vmem_limit_bytes=46 << 20),
        name='muon',
    )(grad, momentum, weight)


def put_kernel(*refs):
    sems = refs[-1]
    copies = [pltpu.make_async_copy(refs[i], refs[3 + i], sems.at[i]) for i in (2, 1, 0)]
    for copy in copies:
        copy.start()
    for copy in copies:
        copy.wait()


def put(*values):
    return pl.pallas_call(
        put_kernel,
        out_shape=tuple(jax.ShapeDtypeStruct(v.shape, v.dtype) for v in values),
        in_specs=[pl.BlockSpec(memory_space=pltpu.VMEM)] * 3,
        out_specs=(pl.BlockSpec(memory_space=pltpu.HBM),) * 3,
        scratch_shapes=[pltpu.SemaphoreType.DMA((3,))],
        compiler_params=pltpu.CompilerParams(vmem_limit_bytes=8 << 20),
        name='put',
    )(*values)


def solution(mesh):
    def local_step(grad_part, momentum, weight):
        grad = grad_part.reshape(RING, RING, RING, 2, SLAB, COLS)
        new_momentum, new_weight, weight_bf16 = put(*muon(grad, *(pltpu.with_memory_space_constraint(v[0], pltpu.HBM) for v in (momentum, weight))))
        return new_momentum[None], new_weight[None], weight_bf16.reshape(1, ROWS, COLS)

    return jax.shard_map(local_step, mesh=mesh, in_specs=(P(('mp', 'dp')), P('mp', 'dp'), P('mp', 'dp')), out_specs=(P('mp', 'dp'), P('mp', 'dp'), P('mp')), check_vma=False)
```

```python
import math
import jax
import jax.numpy as jnp
from jax import lax
from jax.experimental import pallas as pl
from jax.experimental.pallas import tpu as pltpu
from jax.sharding import PartitionSpec as P

MOMENTUM = 0.95
LEARN_RATE = 2.0
WEIGHT_DECAY = 0.25
NS_STEPS = 5
COEF_A = 3.4445
COEF_B = -4.7750
COEF_C = 2.0315

MESH = pl.DeviceIdType.MESH
RING = 4
CHIPS = 64
GROUP = 128
SLAB = 16
COLS = 1024
ROWS = 2048
Z, Y, X = 0, 1, 2
PARTS = ((0, 384, (X, Y, Z)), (384, 384, (Y, Z, X)), (768, 256, (Z, X, Y)))


class Place:
    def __init__(self):
        me = lax.axis_index('dp')
        self.core = lax.rem(me, 2)
        chip = lax.div(me, 2)
        self.xyz = (lax.div(chip, 16), lax.rem(lax.div(chip, 4), 4), lax.rem(chip, 4))

    def index(self, xyz, core):
        return ((xyz[0] * RING + xyz[1]) * RING + xyz[2]) * 2 + core

    def shifted(self, axis, by):
        return lax.rem(self.xyz[axis] + (by % RING), RING)

    def neighbour(self, axis, by):
        xyz = list(self.xyz)
        xyz[axis] = self.shifted(axis, by)
        return {'dp': self.index(xyz, self.core)}

    def partner(self):
        return {'dp': self.index(self.xyz, 1 - self.core)}


def greet(place):
    barrier = pltpu.get_barrier_semaphore()
    peers = [place.partner()] + [place.neighbour(a, s) for a in (Z, Y, X) for s in (1, -1, 2)]
    for peer in peers:
        pl.semaphore_signal(barrier, inc=1, device_id=peer, device_id_type=MESH)
    pl.semaphore_wait(barrier, len(peers))


def at(fixed, rows, cols):
    return tuple(fixed.get(a, slice(None)) for a in (Z, Y, X)) + (rows, cols)


def send(src, dst, ssem, rsem, peer):
    copy = pltpu.make_async_remote_copy(src_ref=src, dst_ref=dst, send_sem=ssem, recv_sem=rsem, device_id=peer, device_id_type=MESH)
    copy.start()
    return copy


ALL = slice(None)
TURNS = (2, 1, -1, 0)


class Line:
    def __init__(self, place, part, phase):
        first, width, order = PARTS[part]
        self.place, self.axis, self.cols = place, order[phase], pl.ds(first, width)
        self.fixed = {a: place.xyz[a] for a in order[:phase]}
        self.free = [a for a in (Z, Y, X) if a in order[phase + 1:]]
        self.next, self.last = (order[1] if phase == 0 else None), order[2]
        self.right, self.left, self.across = (place.neighbour(self.axis, by) for by in (1, -1, 2))

    def narrowed(self, turn, half):
        where = {}
        if turn is not None:
            where[self.next] = self.place.shifted(self.next, turn)
        if half is not None:
            where[self.last] = pl.ds(2 * half, 2)
        return where

    def chunk(self, by, half=None, turn=None):
        return at({**self.fixed, self.axis: self.place.shifted(self.axis, by), **self.narrowed(turn, half)}, ALL, self.cols)

    def slot(self, half=None, turn=None):
        where = self.narrowed(turn, half)
        return (*(where.get(a, ALL) for a in self.free), ALL, self.cols)


def chain_steps(place, acc, ring, rs_ssem, rs_rsem, buf, ag_ssem, ag_rsem, part, ready, update, on_piece, sent):
    outer, middle, inner = (Line(place, part, phase) for phase in range(3))

    def start(bufs, sems, peer, *index):
        copy = send(*bufs, sems[0].at[(part, *index)], sems[1].at[(part, *index)], peer)
        sent.append(copy)
        return copy

    def reduce_send(line, phase, turn, i, where, slot, dst, peer):
        return start((acc.at[where], dst.at[slot]), (rs_ssem, rs_rsem), peer, phase + (turn or 0), i)

    def far_and_own(line, refs, k, turn, ready):
        near_l, near_r, far_l, far_r = refs
        ready(2)
        far = (reduce_send(line, k, 0, 0, line.chunk(2, 0, turn), line.slot(0, turn), far_l, line.right), reduce_send(line, k, 0, 1, line.chunk(2, 1, turn), line.slot(1, turn), far_r, line.left))
        ready(1)
        near = [reduce_send(line, k, 0, 2, line.chunk(1, 1, turn), line.slot(1, turn), near_l, line.right)]
        ready(-1)
        near.append(reduce_send(line, k, 0, 3, line.chunk(-1, 0, turn), line.slot(0, turn), near_r, line.left))
        ready(0)
        return far, near

    def combine(line, refs, k, turn, far, near):
        near_l, near_r, far_l, far_r = refs
        far[0].wait_recv()
        acc[line.chunk(1, 0, turn)] += far_l[line.slot(0, turn)]
        near.append(reduce_send(line, k, 0, 4, line.chunk(1, 0, turn), line.slot(0, turn), near_l, line.right))
        far[1].wait_recv()
        acc[line.chunk(-1, 1, turn)] += far_r[line.slot(1, turn)]
        near.append(reduce_send(line, k, 0, 5, line.chunk(-1, 1, turn), line.slot(1, turn), near_r, line.left))

    def settle(line, refs, turn, near):
        for copy in near:
            copy.wait_recv()
        acc[line.chunk(0, None, turn)] += refs[0][line.slot(None, turn)] + refs[1][line.slot(None, turn)]

    first, second, third = ring[0:4], ring[4:8], ring[8:12]
    state = {}

    def open_turn(k):
        state[k] = far_and_own(outer, first, k, TURNS[k], lambda by: ready(by, k))

    def close_turn(k):
        combine(outer, first, k, TURNS[k], *state[k])

    def end_turn(k):
        settle(outer, first, TURNS[k], state[k][1])

    middle_near = []

    def middle_send(i, by, half, dst, peer):
        return reduce_send(middle, 4, 0, i, middle.chunk(by, half), middle.slot(half), dst, peer)

    open_turn(0)
    yield
    open_turn(1)
    yield
    close_turn(0)
    yield
    open_turn(2)
    yield
    close_turn(1)
    yield
    open_turn(3)
    yield
    close_turn(2)
    yield
    end_turn(0)
    middle_far = (middle_send(0, 2, 0, second[2], middle.right), middle_send(1, 2, 1, second[3], middle.left))
    yield
    close_turn(3)
    yield
    end_turn(1)
    middle_near.append(middle_send(2, 1, 1, second[0], middle.right))
    yield
    end_turn(2)
    middle_near.append(middle_send(3, -1, 0, second[1], middle.left))
    yield
    combine(middle, second, 4, None, middle_far, middle_near)
    yield
    end_turn(3)
    yield
    settle(middle, second, None, middle_near)
    near_l, near_r, far_l, _ = third
    slot = inner.slot()
    copies = [reduce_send(inner, 5, 0, i, inner.chunk(by), slot, dst, peer) for i, by, dst, peer in ((0, 2, far_l, inner.across), (1, 1, near_l, inner.right), (2, -1, near_r, inner.left))]
    yield
    for copy in copies:
        copy.wait_recv()
    acc[inner.chunk(0)] += near_l[slot] + near_r[slot] + far_l[slot]
    update()

    def go(k, i, where, peer):
        start((buf.at[where], buf.at[where]), (ag_ssem, ag_rsem), peer, k, i)

    def recv(k, i, where):
        there = buf.at[where]
        pltpu.make_async_remote_copy(src_ref=there, dst_ref=there, send_sem=ag_ssem.at[part, k, i], recv_sem=ag_rsem.at[part, k, i], device_id=inner.right, device_id_type=MESH).wait_recv()

    def spread(k):
        where = outer.chunk(0, None, TURNS[k])
        go(k, 0, where, outer.right)
        go(k, 1, where, outer.left)
        on_piece(k, 0, where)

    def pass_on(k):
        turn = TURNS[k]
        recv(k, 0, outer.chunk(-1, None, turn))
        go(k, 2, outer.chunk(-1, 0, turn), outer.right)
        on_piece(k, 1, outer.chunk(-1, None, turn))
        recv(k, 1, outer.chunk(1, None, turn))
        go(k, 3, outer.chunk(1, 1, turn), outer.left)
        on_piece(k, 2, outer.chunk(1, None, turn))

    def take(k):
        for half in (0, 1):
            where = outer.chunk(2, half, TURNS[k])
            recv(k, 2 + half, where)
            on_piece(k, 3 + half, where)

    for i, peer in enumerate((inner.across, inner.right, inner.left)):
        go(5, i, inner.chunk(0), peer)
    yield
    for i, by in ((1, -1), (2, 1), (0, 2)):
        recv(5, i, inner.chunk(by))
    for i, half, peer in ((0, 0, middle.right), (1, 1, middle.left), (2, 1, middle.right), (3, 0, middle.left)):
        go(4, i, middle.chunk(0, half), peer)
    spread(3)
    yield
    recv(4, 0, middle.chunk(-1, 0))
    go(4, 4, middle.chunk(-1, 0), middle.right)
    recv(4, 1, middle.chunk(1, 1))
    go(4, 5, middle.chunk(1, 1), middle.left)
    yield
    recv(4, 2, middle.chunk(-1, 1))
    spread(2)
    recv(4, 3, middle.chunk(1, 0))
    spread(1)
    yield
    pass_on(3)
    yield
    recv(4, 4, middle.chunk(2, 0))
    recv(4, 5, middle.chunk(2, 1))
    spread(0)
    yield
    pass_on(2)
    pass_on(1)
    yield
    take(3)
    yield
    pass_on(0)
    yield
    take(2)
    take(1)
    yield
    take(0)


def run_chains(chains):
    while chains:
        chains = [chain for chain in chains if next(chain, chain) is not chain]


NT = (((1,), (1,)), ((), ()))
BLK = 256
NBLK = COLS // BLK


WIDE = 512


def dot_nt(a, b):
    return lax.dot_general(a, b, NT, preferred_element_type=jnp.float32)


def square(n):
    return slice((n % 2) * WIDE, (n % 2 + 1) * WIDE), slice((n // 2) * WIDE, (n // 2 + 1) * WIDE)


def dot(a, b):
    return jnp.dot(a, b, preferred_element_type=jnp.float32)


def weight_step(place, weight, full, ssem, rsem, step):
    def piece(part, phase, i):
        first, width, order = PARTS[part]
        axis = order[phase]
        cols = pl.ds(first, width)
        fixed = {a: place.xyz[a] for a in order[:phase]}
        free = [a for a in (Z, Y, X) if a in order[phase + 1:]]
        right, left, across = place.neighbour(axis, 1), place.neighbour(axis, -1), place.neighbour(axis, 2)

        def chunk(by, half=None):
            where = {**fixed, axis: place.shifted(axis, by)}
            if half is not None:
                where[free[0]] = pl.ds(2 * half, 2)
            return full.at[at(where, ALL, cols)]

        if not free:
            src_by, half, peer, from_by = ((0, None, right, -1), (0, None, left, 1), (0, None, across, 2))[i]
        else:
            src_by, half, peer, from_by = ((0, None, right, -1), (0, None, left, 1), (-1, 0, right, 2), (1, 1, left, 2))[i]
        out = chunk(src_by, half)
        src = weight.at[:, cols] if not free else out
        go = lambda: pltpu.make_async_remote_copy(src_ref=src, dst_ref=out, send_sem=ssem.at[part, phase, i], recv_sem=rsem.at[part, phase, i], device_id=peer, device_id_type=MESH)
        came = chunk(from_by, half)
        come = lambda: pltpu.make_async_remote_copy(src_ref=came, dst_ref=came, send_sem=ssem.at[part, phase, i], recv_sem=rsem.at[part, phase, i], device_id=peer, device_id_type=MESH)
        return go, come

    plan = {0: ((), (2, (0, 1, 2))), 1: ((2, (0, 1, 2)), (1, (0, 1))), 2: ((1, (0, 1)), (1, (2, 3))), 3: ((1, (2, 3)), (0, (0, 1))), 4: ((0, (0, 1)), (0, (2, 3))), 5: ((0, (2, 3)), ())}
    waits, sends = plan[step]
    if waits:
        for i in waits[1]:
            for part in range(3):
                piece(part, waits[0], i)[1]().wait_recv()
    if sends:
        for i in sends[1]:
            for part in range(3):
                piece(part, sends[0], i)[0]().start()
    if step == 5:
        for phase, count in ((2, 3), (1, 4), (0, 4)):
            for i in range(count):
                for part in range(3):
                    piece(part, phase, i)[0]().wait_send()


def muon_kernel(grad, momentum, weight, new_momentum, new_weight, weight_bf16, mine, other, acc, half, xm, xo, gram, poly, part_gram, full, old_mom, old_weight, *scratch):
    ring = scratch[:12]
    load_sem, pair_ssem, pair_rsem, rs_ssem, rs_rsem, ag_ssem, ag_rsem, fw_ssem, fw_rsem, wg_ssem, wg_rsem, xc_ssem, xc_rsem, po_ssem, po_rsem, in_sem = scratch[12:]
    place = Place()
    z, y, x = place.xyz
    order = [(k, by, p) for k in range(4) for by in TURNS for p in range(3)]
    loads, swaps, sent, forwards = {}, {}, [], []

    def block(k, by, p):
        first, width, (outer, middle, _) = PARTS[p]
        return at({outer: place.shifted(outer, by), middle: place.shifted(middle, TURNS[k])}, ALL, pl.ds(first, width))

    for k, by, p in order:
        bz, bly, bx, r, c = here = block(k, by, p)
        loads[p, k, by] = pltpu.make_async_copy(grad.at[bz, bly, bx, place.core, r, c], acc.at[here], load_sem.at[p, k, TURNS.index(by)])
        loads[p, k, by].start()
    into = (pltpu.make_async_copy(momentum, old_mom, in_sem.at[0]), pltpu.make_async_copy(weight, old_weight, in_sem.at[1]))
    for copy in into:
        copy.start()
    greet(place)
    for k, by, p in order:
        bz, bly, bx, r, c = here = block(k, by, p)
        swaps[p, k, by] = send(grad.at[bz, bly, bx, 1 - place.core, r, c], half.at[here], pair_ssem.at[p, k, TURNS.index(by)], pair_rsem.at[p, k, TURNS.index(by)], place.partner())
    for copy in into:
        copy.wait()
    full[z, y, x] = old_weight[...]
    wstep = lambda i: weight_step(place, old_weight, full, wg_ssem, wg_rsem, i)
    wstep(0)

    def chain(p):
        cols = pl.ds(*PARTS[p][:2])

        def ready(by, k):
            here = block(k, by, p)
            loads[p, k, by].wait()
            swaps[p, k, by].wait_recv()
            acc[here] += half[here]

        def update():
            g = acc[z, y, x, :, cols] / GROUP
            mom = MOMENTUM * old_mom[:, cols] + g
            new_momentum[:, cols] = mom
            mine[z, y, x, :, cols] = (g + MOMENTUM * mom).astype(jnp.bfloat16)

        def forward(k, i, where):
            forwards.append(send(mine.at[where], other.at[where], fw_ssem.at[p, k, i], fw_rsem.at[p, k, i], place.partner()))

        return chain_steps(place, acc, ring, rs_ssem, rs_rsem, mine, ag_ssem, ag_rsem, p, ready, update, forward, sent)

    run_chains([chain(p) for p in range(3)])
    wstep(1)

    def squares(buf, total):
        for i in range(RING):
            block = buf[i].reshape(BLK // 8, 8, COLS).astype(jnp.float32)
            total += jnp.sum(block * block, axis=0)
        return total

    total = squares(mine, jnp.zeros((8, COLS), jnp.float32))
    for copy in forwards:
        copy.wait_recv()
    total = squares(other, total)
    for copy in sent + forwards + list(swaps.values()):
        copy.wait_send()
    norm = jnp.sqrt(jnp.sum(jnp.sum(total, axis=0, keepdims=True), axis=1, keepdims=True))
    inverse = 1.0 / (norm + 1e-7)
    for buf, dst in ((mine, xm), (other, xo)):
        for i in range(RING):
            block = (buf[i].reshape(BLK, COLS).astype(jnp.float32) * inverse).astype(jnp.bfloat16)
            dst[0, :, i * BLK:(i + 1) * BLK] = block.T

    def exchange(slot, n):
        rows, cols = square(n)
        return pltpu.make_async_remote_copy(src_ref=xm.at[slot, rows, cols], dst_ref=xo.at[slot, rows, cols], send_sem=xc_ssem.at[slot, n], recv_sem=xc_rsem.at[slot, n], device_id=place.partner(), device_id_type=MESH)

    def mirror(dst, j, tall):
        dst[j * BLK:, j * BLK:(j + 1) * BLK] = tall
        if j < NBLK - 1:
            dst[j * BLK:(j + 1) * BLK, (j + 1) * BLK:] = tall[BLK:].T

    def newton_schulz(t, carry):
        now = lax.rem(t, 2)
        before = 1 - now
        @pl.when(t > 0)
        def _():
            for k in range(2):
                cols = slice(k * WIDE, (k + 1) * WIDE)
                old = xm[before, :, cols]
                xm[now, :, cols] = (COEF_A * old.astype(jnp.float32) + dot(poly[...], old)).astype(jnp.bfloat16)
                exchange(now, 2 * k).start()
                exchange(now, 2 * k + 1).start()

        for j in range(NBLK):
            rows = slice(j * BLK, COLS)
            part_gram[rows, j * BLK:(j + 1) * BLK] = dot_nt(xm[now, rows], xm[now, j * BLK:(j + 1) * BLK])

        for k in range(2):
            @pl.when(t > 0)
            def _():
                for n in (2 * k, 2 * k + 1):
                    exchange(now, n).wait()

            deep = slice(k * WIDE, (k + 1) * WIDE)
            for j in range(NBLK):
                rows, cols = slice(j * BLK, COLS), slice(j * BLK, (j + 1) * BLK)
                tall = part_gram[rows, cols] + dot_nt(xo[now, rows, deep], xo[now, cols, deep])
                if k == 0:
                    part_gram[rows, cols] = tall
                else:
                    mirror(gram, j, tall.astype(jnp.bfloat16))
        for j in range(NBLK):
            rows, cols = slice(j * BLK, COLS), slice(j * BLK, (j + 1) * BLK)
            tall = COEF_B * gram[rows, cols].astype(jnp.float32) + COEF_C * dot_nt(gram[rows, :], gram[cols, :])
            mirror(poly, j, tall.astype(jnp.bfloat16))

        for when, step in ((0, 2), (1, 3), (3, 4)):
            @pl.when(t == when)
            def _():
                wstep(step)
        return carry

    lax.fori_loop(0, NS_STEPS, newton_schulz, 0)
    last = (NS_STEPS - 1) % 2
    scale = 0.2 * math.sqrt(ROWS)
    outs = []
    for n in range(NBLK):
        if n % 2 == 0:
            cols = slice(n * BLK, n * BLK + WIDE)
            old = xm[last, :, cols]
            pair = (COEF_A * old.astype(jnp.float32) + dot(poly[...], old)).astype(jnp.bfloat16)
        if n == 0:
            wstep(5)
        ortho = pair[:, (n % 2) * BLK:(n % 2 + 1) * BLK]
        w = full[n]
        w = w - LEARN_RATE * (scale * ortho.T.astype(jnp.float32).reshape(w.shape) + WEIGHT_DECAY * w)
        full[n] = w
        weight_bf16[n, :, :, place.core] = w.astype(jnp.bfloat16)
        there = weight_bf16.at[n, :, :, place.core]
        outs.append(send(there, there, po_ssem.at[n], po_rsem.at[n], place.partner()))
    new_weight[...] = full[z, y, x]
    for copy in outs:
        copy.wait()


def muon(grad, momentum, weight):
    ring = []
    for lead in ((RING, RING), (RING,), ()):
        ring += [pltpu.VMEM(lead + (SLAB, COLS), jnp.float32)] * 4
    dma = pltpu.SemaphoreType.DMA
    cube = (RING, RING, RING, SLAB, COLS)
    vmem = pl.BlockSpec(memory_space=pltpu.VMEM)
    hbm = pl.BlockSpec(memory_space=pltpu.HBM)
    anywhere = pl.BlockSpec(memory_space=pl.ANY)
    f32, bf16 = jnp.float32, jnp.bfloat16
    return pl.pallas_call(
        muon_kernel,
        out_shape=(jax.ShapeDtypeStruct((SLAB, COLS), f32), jax.ShapeDtypeStruct((SLAB, COLS), f32), jax.ShapeDtypeStruct((RING, RING, RING, 2, SLAB, COLS), bf16)),
        in_specs=[anywhere, hbm, hbm],
        out_specs=(vmem, vmem, vmem),
        scratch_shapes=[pltpu.VMEM(cube, bf16), pltpu.VMEM(cube, bf16), pltpu.VMEM(cube, f32), pltpu.VMEM(cube, f32),
                        pltpu.VMEM((2, COLS, COLS), bf16), pltpu.VMEM((2, COLS, COLS), bf16), pltpu.VMEM((COLS, COLS), bf16), pltpu.VMEM((COLS, COLS), bf16),
                        pltpu.VMEM((COLS, COLS), f32), pltpu.VMEM(cube, f32), pltpu.VMEM((SLAB, COLS), f32), pltpu.VMEM((SLAB, COLS), f32), *ring,
                        *[dma((3, 4, 4))] * 3, *[dma((3, 6, 6))] * 4, *[dma((3, 4, 5))] * 2,
                        dma((3, 3, 4)), dma((3, 3, 4)), dma((2, NBLK)), dma((2, NBLK)), dma((NBLK,)), dma((NBLK,)), dma((2,))],
        compiler_params=pltpu.CompilerParams(collective_id=0, has_side_effects=True, vmem_limit_bytes=46 << 20),
        name='muon',
    )(grad, momentum, weight)


def put_kernel(*refs):
    sems = refs[-1]
    copies = [pltpu.make_async_copy(refs[i], refs[3 + i], sems.at[i]) for i in (2, 1, 0)]
    for copy in copies:
        copy.start()
    for copy in copies:
        copy.wait()


def put(*values):
    return pl.pallas_call(
        put_kernel,
        out_shape=tuple(jax.ShapeDtypeStruct(v.shape, v.dtype) for v in values),
        in_specs=[pl.BlockSpec(memory_space=pltpu.VMEM)] * 3,
        out_specs=(pl.BlockSpec(memory_space=pltpu.HBM),) * 3,
        scratch_shapes=[pltpu.SemaphoreType.DMA((3,))],
        compiler_params=pltpu.CompilerParams(vmem_limit_bytes=8 << 20),
        name='put',
    )(*values)


def solution(mesh):
    def local_step(grad_part, momentum, weight):
        grad = grad_part.reshape(RING, RING, RING, 2, SLAB, COLS)
        new_momentum, new_weight, weight_bf16 = put(*muon(grad, *(pltpu.with_memory_space_constraint(v[0], pltpu.HBM) for v in (momentum, weight))))
        return new_momentum[None], new_weight[None], weight_bf16.reshape(1, ROWS, COLS)

    return jax.shard_map(local_step, mesh=mesh, in_specs=(P(('mp', 'dp')), P('mp', 'dp'), P('mp', 'dp')), out_specs=(P('mp', 'dp'), P('mp', 'dp'), P('mp')), check_vma=False)
```

```python
import math
import jax
import jax.numpy as jnp
from jax import lax
from jax.experimental import pallas as pl
from jax.experimental.pallas import tpu as pltpu
from jax.sharding import PartitionSpec as P

MOMENTUM = 0.95
LEARN_RATE = 2.0
WEIGHT_DECAY = 0.25
NS_STEPS = 5
COEF_A = 3.4445
COEF_B = -4.7750
COEF_C = 2.0315

MESH = pl.DeviceIdType.MESH
RING = 4
CHIPS = 64
GROUP = 128
SLAB = 16
COLS = 1024
ROWS = 2048
Z, Y, X = 0, 1, 2
PARTS = ((0, 384, (X, Y, Z)), (384, 384, (Y, Z, X)), (768, 256, (Z, X, Y)))


class Place:
    def __init__(self):
        me = lax.axis_index('dp')
        self.core = lax.rem(me, 2)
        chip = lax.div(me, 2)
        self.xyz = (lax.div(chip, 16), lax.rem(lax.div(chip, 4), 4), lax.rem(chip, 4))

    def index(self, xyz, core):
        return ((xyz[0] * RING + xyz[1]) * RING + xyz[2]) * 2 + core

    def shifted(self, axis, by):
        return lax.rem(self.xyz[axis] + (by % RING), RING)

    def neighbour(self, axis, by):
        xyz = list(self.xyz)
        xyz[axis] = self.shifted(axis, by)
        return {'dp': self.index(xyz, self.core)}

    def partner(self):
        return {'dp': self.index(self.xyz, 1 - self.core)}


def greet(place):
    barrier = pltpu.get_barrier_semaphore()
    peers = [place.partner()] + [place.neighbour(a, s) for a in (Z, Y, X) for s in (1, -1, 2)]
    for peer in peers:
        pl.semaphore_signal(barrier, inc=1, device_id=peer, device_id_type=MESH)
    pl.semaphore_wait(barrier, len(peers))


def at(fixed, rows, cols):
    return tuple(fixed.get(a, slice(None)) for a in (Z, Y, X)) + (rows, cols)


def send(src, dst, ssem, rsem, peer):
    copy = pltpu.make_async_remote_copy(src_ref=src, dst_ref=dst, send_sem=ssem, recv_sem=rsem, device_id=peer, device_id_type=MESH)
    copy.start()
    return copy


ALL = slice(None)
TURNS = (2, 1, -1, 0)


class Line:
    def __init__(self, place, part, phase):
        first, width, order = PARTS[part]
        self.place, self.axis, self.cols = place, order[phase], pl.ds(first, width)
        self.fixed = {a: place.xyz[a] for a in order[:phase]}
        self.free = [a for a in (Z, Y, X) if a in order[phase + 1:]]
        self.next, self.last = (order[1] if phase == 0 else None), order[2]
        self.right, self.left, self.across = (place.neighbour(self.axis, by) for by in (1, -1, 2))

    def narrowed(self, turn, half):
        where = {}
        if turn is not None:
            where[self.next] = self.place.shifted(self.next, turn)
        if half is not None:
            where[self.last] = pl.ds(2 * half, 2)
        return where

    def chunk(self, by, half=None, turn=None):
        return at({**self.fixed, self.axis: self.place.shifted(self.axis, by), **self.narrowed(turn, half)}, ALL, self.cols)

    def slot(self, half=None, turn=None):
        where = self.narrowed(turn, half)
        return (*(where.get(a, ALL) for a in self.free), ALL, self.cols)


def chain_steps(place, acc, ring, rs_ssem, rs_rsem, buf, ag_ssem, ag_rsem, part, ready, update, on_piece, sent):
    outer, middle, inner = (Line(place, part, phase) for phase in range(3))

    def start(bufs, sems, peer, *index):
        copy = send(*bufs, sems[0].at[(part, *index)], sems[1].at[(part, *index)], peer)
        sent.append(copy)
        return copy

    def reduce_send(line, phase, turn, i, where, slot, dst, peer):
        return start((acc.at[where], dst.at[slot]), (rs_ssem, rs_rsem), peer, phase + (turn or 0), i)

    def far_and_own(line, refs, k, turn, ready):
        near_l, near_r, far_l, far_r = refs
        ready(2)
        far = (reduce_send(line, k, 0, 0, line.chunk(2, 0, turn), line.slot(0, turn), far_l, line.right), reduce_send(line, k, 0, 1, line.chunk(2, 1, turn), line.slot(1, turn), far_r, line.left))
        ready(1)
        near = [reduce_send(line, k, 0, 2, line.chunk(1, 1, turn), line.slot(1, turn), near_l, line.right)]
        ready(-1)
        near.append(reduce_send(line, k, 0, 3, line.chunk(-1, 0, turn), line.slot(0, turn), near_r, line.left))
        ready(0)
        return far, near

    def combine(line, refs, k, turn, far, near):
        near_l, near_r, far_l, far_r = refs
        far[0].wait_recv()
        acc[line.chunk(1, 0, turn)] += far_l[line.slot(0, turn)]
        near.append(reduce_send(line, k, 0, 4, line.chunk(1, 0, turn), line.slot(0, turn), near_l, line.right))
        far[1].wait_recv()
        acc[line.chunk(-1, 1, turn)] += far_r[line.slot(1, turn)]
        near.append(reduce_send(line, k, 0, 5, line.chunk(-1, 1, turn), line.slot(1, turn), near_r, line.left))

    def settle(line, refs, turn, near):
        for copy in near:
            copy.wait_recv()
        acc[line.chunk(0, None, turn)] += refs[0][line.slot(None, turn)] + refs[1][line.slot(None, turn)]

    first, second, third = ring[0:4], ring[4:8], ring[8:12]
    state = {}

    def open_turn(k):
        state[k] = far_and_own(outer, first, k, TURNS[k], lambda by: ready(by, k))

    def close_turn(k):
        combine(outer, first, k, TURNS[k], *state[k])

    def end_turn(k):
        settle(outer, first, TURNS[k], state[k][1])

    middle_near = []

    def middle_send(i, by, half, dst, peer):
        return reduce_send(middle, 4, 0, i, middle.chunk(by, half), middle.slot(half), dst, peer)

    open_turn(0)
    yield
    open_turn(1)
    yield
    close_turn(0)
    yield
    open_turn(2)
    yield
    close_turn(1)
    yield
    open_turn(3)
    yield
    close_turn(2)
    yield
    end_turn(0)
    middle_far = (middle_send(0, 2, 0, second[2], middle.right), middle_send(1, 2, 1, second[3], middle.left))
    yield
    close_turn(3)
    yield
    end_turn(1)
    middle_near.append(middle_send(2, 1, 1, second[0], middle.right))
    yield
    end_turn(2)
    middle_near.append(middle_send(3, -1, 0, second[1], middle.left))
    yield
    combine(middle, second, 4, None, middle_far, middle_near)
    yield
    end_turn(3)
    yield
    settle(middle, second, None, middle_near)
    near_l, near_r, far_l, _ = third
    slot = inner.slot()
    copies = [reduce_send(inner, 5, 0, i, inner.chunk(by), slot, dst, peer) for i, by, dst, peer in ((0, 2, far_l, inner.across), (1, 1, near_l, inner.right), (2, -1, near_r, inner.left))]
    yield
    for copy in copies:
        copy.wait_recv()
    acc[inner.chunk(0)] += near_l[slot] + near_r[slot] + far_l[slot]
    update()

    def go(k, i, where, peer):
        start((buf.at[where], buf.at[where]), (ag_ssem, ag_rsem), peer, k, i)

    def recv(k, i, where):
        there = buf.at[where]
        pltpu.make_async_remote_copy(src_ref=there, dst_ref=there, send_sem=ag_ssem.at[part, k, i], recv_sem=ag_rsem.at[part, k, i], device_id=inner.right, device_id_type=MESH).wait_recv()

    def spread(k):
        where = outer.chunk(0, None, TURNS[k])
        go(k, 0, where, outer.right)
        go(k, 1, where, outer.left)
        on_piece(k, 0, where)

    def pass_on(k):
        turn = TURNS[k]
        recv(k, 0, outer.chunk(-1, None, turn))
        go(k, 2, outer.chunk(-1, 0, turn), outer.right)
        on_piece(k, 1, outer.chunk(-1, None, turn))
        recv(k, 1, outer.chunk(1, None, turn))
        go(k, 3, outer.chunk(1, 1, turn), outer.left)
        on_piece(k, 2, outer.chunk(1, None, turn))

    def take(k):
        for half in (0, 1):
            where = outer.chunk(2, half, TURNS[k])
            recv(k, 2 + half, where)
            on_piece(k, 3 + half, where)

    for i, peer in enumerate((inner.across, inner.right, inner.left)):
        go(5, i, inner.chunk(0), peer)
    yield
    for i, by in ((1, -1), (2, 1), (0, 2)):
        recv(5, i, inner.chunk(by))
    for i, half, peer in ((0, 0, middle.right), (1, 1, middle.left), (2, 1, middle.right), (3, 0, middle.left)):
        go(4, i, middle.chunk(0, half), peer)
    spread(3)
    yield
    recv(4, 0, middle.chunk(-1, 0))
    go(4, 4, middle.chunk(-1, 0), middle.right)
    recv(4, 1, middle.chunk(1, 1))
    go(4, 5, middle.chunk(1, 1), middle.left)
    yield
    recv(4, 2, middle.chunk(-1, 1))
    recv(4, 3, middle.chunk(1, 0))
    yield
    pass_on(3)
    spread(2)
    spread(1)
    yield
    recv(4, 4, middle.chunk(2, 0))
    recv(4, 5, middle.chunk(2, 1))
    spread(0)
    yield
    pass_on(2)
    pass_on(1)
    yield
    take(3)
    yield
    pass_on(0)
    yield
    take(2)
    take(1)
    yield
    take(0)


def run_chains(chains, after_first):
    first = True
    while chains:
        chains = [chain for chain in chains if next(chain, chain) is not chain]
        if first:
            after_first()
        first = False


NT = (((1,), (1,)), ((), ()))
BLK = 256
NBLK = COLS // BLK


WIDE = 512


def dot_nt(a, b):
    return lax.dot_general(a, b, NT, preferred_element_type=jnp.float32)


def square(n):
    return slice((n % 2) * WIDE, (n % 2 + 1) * WIDE), slice((n // 2) * WIDE, (n // 2 + 1) * WIDE)


def dot(a, b):
    return jnp.dot(a, b, preferred_element_type=jnp.float32)


def weight_step(place, weight, full, ssem, rsem, step):
    def piece(part, phase, i):
        first, width, order = PARTS[part]
        axis = order[phase]
        cols = pl.ds(first, width)
        fixed = {a: place.xyz[a] for a in order[:phase]}
        free = [a for a in (Z, Y, X) if a in order[phase + 1:]]
        right, left, across = place.neighbour(axis, 1), place.neighbour(axis, -1), place.neighbour(axis, 2)

        def chunk(by, half=None):
            where = {**fixed, axis: place.shifted(axis, by)}
            if half is not None:
                where[free[0]] = pl.ds(2 * half, 2)
            return full.at[at(where, ALL, cols)]

        if not free:
            src_by, half, peer, from_by = ((0, None, right, -1), (0, None, left, 1), (0, None, across, 2))[i]
        else:
            src_by, half, peer, from_by = ((0, None, right, -1), (0, None, left, 1), (-1, 0, right, 2), (1, 1, left, 2))[i]
        out = chunk(src_by, half)
        src = weight.at[:, cols] if not free else out
        go = lambda: pltpu.make_async_remote_copy(src_ref=src, dst_ref=out, send_sem=ssem.at[part, phase, i], recv_sem=rsem.at[part, phase, i], device_id=peer, device_id_type=MESH)
        came = chunk(from_by, half)
        come = lambda: pltpu.make_async_remote_copy(src_ref=came, dst_ref=came, send_sem=ssem.at[part, phase, i], recv_sem=rsem.at[part, phase, i], device_id=peer, device_id_type=MESH)
        return go, come

    plan = {0: ((), (2, (0, 1, 2))), 1: ((2, (0, 1, 2)), (1, (0, 1))), 2: ((1, (0, 1)), (1, (2, 3))), 3: ((1, (2, 3)), (0, (0, 1))), 4: ((0, (0, 1)), (0, (2, 3))), 5: ((0, (2, 3)), ())}
    waits, sends = plan[step]
    if waits:
        for i in waits[1]:
            for part in range(3):
                piece(part, waits[0], i)[1]().wait_recv()
    if sends:
        for i in sends[1]:
            for part in range(3):
                piece(part, sends[0], i)[0]().start()
    if step == 5:
        for phase, count in ((2, 3), (1, 4), (0, 4)):
            for i in range(count):
                for part in range(3):
                    piece(part, phase, i)[0]().wait_send()


def muon_kernel(grad, momentum, weight, new_momentum, new_weight, weight_bf16, mine, other, acc, half, xm, xo, gram, poly, part_gram, full, old_mom, old_weight, *scratch):
    ring = scratch[:12]
    load_sem, pair_ssem, pair_rsem, rs_ssem, rs_rsem, ag_ssem, ag_rsem, fw_ssem, fw_rsem, wg_ssem, wg_rsem, xc_ssem, xc_rsem, po_ssem, po_rsem, in_sem = scratch[12:]
    place = Place()
    z, y, x = place.xyz
    order = [(k, by, p) for k in range(4) for by in TURNS for p in range(3)]
    loads, swaps, sent, forwards = {}, {}, [], []

    def block(k, by, p):
        first, width, (outer, middle, _) = PARTS[p]
        return at({outer: place.shifted(outer, by), middle: place.shifted(middle, TURNS[k])}, ALL, pl.ds(first, width))

    for k, by, p in order:
        bz, bly, bx, r, c = here = block(k, by, p)
        loads[p, k, by] = pltpu.make_async_copy(grad.at[bz, bly, bx, place.core, r, c], acc.at[here], load_sem.at[p, k, TURNS.index(by)])
        loads[p, k, by].start()
    into = (pltpu.make_async_copy(momentum, old_mom, in_sem.at[0]), pltpu.make_async_copy(weight, old_weight, in_sem.at[1]))
    for copy in into:
        copy.start()
    greet(place)
    for k, by, p in order:
        bz, bly, bx, r, c = here = block(k, by, p)
        swaps[p, k, by] = send(grad.at[bz, bly, bx, 1 - place.core, r, c], half.at[here], pair_ssem.at[p, k, TURNS.index(by)], pair_rsem.at[p, k, TURNS.index(by)], place.partner())
    wstep = lambda i: weight_step(place, old_weight, full, wg_ssem, wg_rsem, i)

    def first_turn_out():
        for copy in into:
            copy.wait()
        full[z, y, x] = old_weight[...]
        wstep(0)

    def chain(p):
        cols = pl.ds(*PARTS[p][:2])

        def ready(by, k):
            here = block(k, by, p)
            loads[p, k, by].wait()
            swaps[p, k, by].wait_recv()
            acc[here] += half[here]

        def update():
            g = acc[z, y, x, :, cols] / GROUP
            mom = MOMENTUM * old_mom[:, cols] + g
            new_momentum[:, cols] = mom
            mine[z, y, x, :, cols] = (g + MOMENTUM * mom).astype(jnp.bfloat16)

        def forward(k, i, where):
            forwards.append(send(mine.at[where], other.at[where], fw_ssem.at[p, k, i], fw_rsem.at[p, k, i], place.partner()))

        return chain_steps(place, acc, ring, rs_ssem, rs_rsem, mine, ag_ssem, ag_rsem, p, ready, update, forward, sent)

    run_chains([chain(p) for p in range(3)], first_turn_out)
    wstep(1)

    def squares(buf, total):
        for i in range(RING):
            block = buf[i].reshape(BLK // 8, 8, COLS).astype(jnp.float32)
            total += jnp.sum(block * block, axis=0)
        return total

    total = squares(mine, jnp.zeros((8, COLS), jnp.float32))
    for copy in forwards:
        copy.wait_recv()
    total = squares(other, total)
    for copy in sent + forwards + list(swaps.values()):
        copy.wait_send()
    norm = jnp.sqrt(jnp.sum(jnp.sum(total, axis=0, keepdims=True), axis=1, keepdims=True))
    inverse = 1.0 / (norm + 1e-7)
    for buf, dst in ((mine, xm), (other, xo)):
        for i in range(RING):
            block = (buf[i].reshape(BLK, COLS).astype(jnp.float32) * inverse).astype(jnp.bfloat16)
            dst[0, :, i * BLK:(i + 1) * BLK] = block.T

    def exchange(slot, n):
        rows, cols = square(n)
        return pltpu.make_async_remote_copy(src_ref=xm.at[slot, rows, cols], dst_ref=xo.at[slot, rows, cols], send_sem=xc_ssem.at[slot, n], recv_sem=xc_rsem.at[slot, n], device_id=place.partner(), device_id_type=MESH)

    def mirror(dst, j, tall):
        dst[j * BLK:, j * BLK:(j + 1) * BLK] = tall
        if j < NBLK - 1:
            dst[j * BLK:(j + 1) * BLK, (j + 1) * BLK:] = tall[BLK:].T

    def newton_schulz(t, carry):
        now = lax.rem(t, 2)
        before = 1 - now
        @pl.when(t > 0)
        def _():
            for k in range(2):
                cols = slice(k * WIDE, (k + 1) * WIDE)
                old = xm[before, :, cols]
                xm[now, :, cols] = (COEF_A * old.astype(jnp.float32) + dot(poly[...], old)).astype(jnp.bfloat16)
                exchange(now, 2 * k).start()
                exchange(now, 2 * k + 1).start()

        for j in range(NBLK):
            rows = slice(j * BLK, COLS)
            part_gram[rows, j * BLK:(j + 1) * BLK] = dot_nt(xm[now, rows], xm[now, j * BLK:(j + 1) * BLK])

        for k in range(2):
            @pl.when(t > 0)
            def _():
                for n in (2 * k, 2 * k + 1):
                    exchange(now, n).wait()

            deep = slice(k * WIDE, (k + 1) * WIDE)
            for j in range(NBLK):
                rows, cols = slice(j * BLK, COLS), slice(j * BLK, (j + 1) * BLK)
                tall = part_gram[rows, cols] + dot_nt(xo[now, rows, deep], xo[now, cols, deep])
                if k == 0:
                    part_gram[rows, cols] = tall
                else:
                    mirror(gram, j, tall.astype(jnp.bfloat16))
        for j in range(NBLK):
            rows, cols = slice(j * BLK, COLS), slice(j * BLK, (j + 1) * BLK)
            tall = COEF_B * gram[rows, cols].astype(jnp.float32) + COEF_C * dot_nt(gram[rows, :], gram[cols, :])
            mirror(poly, j, tall.astype(jnp.bfloat16))

        for when, step in ((0, 2), (1, 3), (3, 4)):
            @pl.when(t == when)
            def _():
                wstep(step)
        return carry

    lax.fori_loop(0, NS_STEPS, newton_schulz, 0)
    last = (NS_STEPS - 1) % 2
    scale = 0.2 * math.sqrt(ROWS)
    outs = []
    for n in range(NBLK):
        if n % 2 == 0:
            cols = slice(n * BLK, n * BLK + WIDE)
            old = xm[last, :, cols]
            pair = (COEF_A * old.astype(jnp.float32) + dot(poly[...], old)).astype(jnp.bfloat16)
        if n == 0:
            wstep(5)
        ortho = pair[:, (n % 2) * BLK:(n % 2 + 1) * BLK]
        w = full[n]
        w = w - LEARN_RATE * (scale * ortho.T.astype(jnp.float32).reshape(w.shape) + WEIGHT_DECAY * w)
        full[n] = w
        weight_bf16[n, :, :, place.core] = w.astype(jnp.bfloat16)
        there = weight_bf16.at[n, :, :, place.core]
        outs.append(send(there, there, po_ssem.at[n], po_rsem.at[n], place.partner()))
    new_weight[...] = full[z, y, x]
    for copy in outs:
        copy.wait()


def muon(grad, momentum, weight):
    ring = []
    for lead in ((RING, RING), (RING,), ()):
        ring += [pltpu.VMEM(lead + (SLAB, COLS), jnp.float32)] * 4
    dma = pltpu.SemaphoreType.DMA
    cube = (RING, RING, RING, SLAB, COLS)
    vmem = pl.BlockSpec(memory_space=pltpu.VMEM)
    hbm = pl.BlockSpec(memory_space=pltpu.HBM)
    anywhere = pl.BlockSpec(memory_space=pl.ANY)
    f32, bf16 = jnp.float32, jnp.bfloat16
    return pl.pallas_call(
        muon_kernel,
        out_shape=(jax.ShapeDtypeStruct((SLAB, COLS), f32), jax.ShapeDtypeStruct((SLAB, COLS), f32), jax.ShapeDtypeStruct((RING, RING, RING, 2, SLAB, COLS), bf16)),
        in_specs=[anywhere, hbm, hbm],
        out_specs=(vmem, vmem, vmem),
        scratch_shapes=[pltpu.VMEM(cube, bf16), pltpu.VMEM(cube, bf16), pltpu.VMEM(cube, f32), pltpu.VMEM(cube, f32),
                        pltpu.VMEM((2, COLS, COLS), bf16), pltpu.VMEM((2, COLS, COLS), bf16), pltpu.VMEM((COLS, COLS), bf16), pltpu.VMEM((COLS, COLS), bf16),
                        pltpu.VMEM((COLS, COLS), f32), pltpu.VMEM(cube, f32), pltpu.VMEM((SLAB, COLS), f32), pltpu.VMEM((SLAB, COLS), f32), *ring,
                        *[dma((3, 4, 4))] * 3, *[dma((3, 6, 6))] * 4, *[dma((3, 4, 5))] * 2,
                        dma((3, 3, 4)), dma((3, 3, 4)), dma((2, NBLK)), dma((2, NBLK)), dma((NBLK,)), dma((NBLK,)), dma((2,))],
        compiler_params=pltpu.CompilerParams(collective_id=0, has_side_effects=True, vmem_limit_bytes=46 << 20),
        name='muon',
    )(grad, momentum, weight)


def put_kernel(*refs):
    sems = refs[-1]
    copies = [pltpu.make_async_copy(refs[i], refs[3 + i], sems.at[i]) for i in (2, 1, 0)]
    for copy in copies:
        copy.start()
    for copy in copies:
        copy.wait()


def put(*values):
    return pl.pallas_call(
        put_kernel,
        out_shape=tuple(jax.ShapeDtypeStruct(v.shape, v.dtype) for v in values),
        in_specs=[pl.BlockSpec(memory_space=pltpu.VMEM)] * 3,
        out_specs=(pl.BlockSpec(memory_space=pltpu.HBM),) * 3,
        scratch_shapes=[pltpu.SemaphoreType.DMA((3,))],
        compiler_params=pltpu.CompilerParams(vmem_limit_bytes=8 << 20),
        name='put',
    )(*values)


def solution(mesh):
    def local_step(grad_part, momentum, weight):
        grad = grad_part.reshape(RING, RING, RING, 2, SLAB, COLS)
        new_momentum, new_weight, weight_bf16 = put(*muon(grad, *(pltpu.with_memory_space_constraint(v[0], pltpu.HBM) for v in (momentum, weight))))
        return new_momentum[None], new_weight[None], weight_bf16.reshape(1, ROWS, COLS)

    return jax.shard_map(local_step, mesh=mesh, in_specs=(P(('mp', 'dp')), P('mp', 'dp'), P('mp', 'dp')), out_specs=(P('mp', 'dp'), P('mp', 'dp'), P('mp')), check_vma=False)
```
